256 devices in a mesh: dp: 8 (over x, core), band: 32 (over y, z).
Axes of the slice: x: 4, y: 4, z: 8, core: 2. Of those that a mesh axis runs over, the one named last changes fastest.
Arguments:
- features: bfloat16 [65280, 256], P(('dp', 'band')), parts along dimension 0, may hold values from -6 to 6
- corners: int32 [65280, 512], P(('dp', 'band')), parts along dimension 0, may hold values from 0 to 6143, as said below
- bilinear: float32 [65280, 512], P(('dp', 'band')), parts along dimension 0, may hold values from 0.08 to 0.5, as said below
- attention: float32 [65280, 128], P(('dp', 'band')), parts along dimension 0, may hold values from 0 to 1, as said below
- w_value: bfloat16 [256, 256], replicated, may hold values from -0.375 to 0.375
- b_value: float32 [256], replicated, may hold values from -0.6 to 0.6
- w_out: bfloat16 [256, 256], replicated, may hold values from -1.5 to 1.5
- b_out: float32 [256], replicated, may hold values from -3 to 3
- norm1_gain: float32 [256], replicated, may hold values from 0.5 to 1.5
- norm1_bias: float32 [256], replicated, may hold values from -3 to 3
- w_in: bfloat16 [256, 1024], replicated, may hold values from -0.375 to 0.375
- b_in: float32 [1024], replicated, may hold values from -3 to 3
- w_ffout: bfloat16 [1024, 256], replicated, may hold values from -0.1875 to 0.1875
- b_ffout: float32 [256], replicated, may hold values from -3 to 3
- norm2_gain: float32 [256], replicated, may hold values from 0.5 to 1.5
- norm2_bias: float32 [256], replicated, may hold values from -3 to 3
Outputs:
- encoded: bfloat16 [65280, 256], P(('dp', 'band')), parts along dimension 0
The draws below stay inside these ranges and needn't reach their ends.
There are 8 independent parts, one for each index of `dp`. The reference program is written for one: setup_inputs(seed, part) draws one part's arguments, and reference() takes and returns one part's arrays. A program takes and returns all parts, laid end to end along the dimension named above; an argument that names none is the same for every part. Nothing has to cross between parts.
Inputs may be any that keep to these rules, and one draw needn't show every extreme that they name: An entry for level l is a row of a map of 192 * 32 // 4**l tokens laid out in rows of 128 // 2**l; the four corners of a point are k, k + 1, k + 128 // 2**l and k + 128 // 2**l + 1 in that order. `bilinear`: the four corner weights of a point are positive and sum to one. `attention`: for each token and head the 16 weights are positive and sum to one.
All inputs are finite; a program needn't handle non-finite values.
Results may differ from the reference program's by a relative error of at most 0.009.
Values may be sent and summed in bfloat16 or wider, within the bound.
A program may use at most 64 MiB of HBM per device.

```python
import jax
import jax.numpy as jnp
from jax import lax

D = 256
HEADS = 8
FF = 1024
LEVELS = 4
POINTS = 4
MAP_W = 128
ROWS_DEV = 192
BAND_ROWS = 255
TOKENS = 8160


def query_place():
    band_total = TOKENS // BAND_ROWS
    token_ids = jnp.arange(TOKENS, dtype=jnp.int32)
    band_index = token_ids // BAND_ROWS
    local_row = token_ids % BAND_ROWS
    own_position = band_index * ROWS_DEV + local_row
    own_length = jnp.zeros((TOKENS,), jnp.int32) + ROWS_DEV * band_total
    offset_rows = 0
    for level_index in range(LEVELS):
        rows_here = ROWS_DEV // 4 ** level_index
        inside = (local_row >= offset_rows) & (local_row < offset_rows + rows_here)
        own_position = jnp.where(inside, band_index * rows_here + local_row - offset_rows, own_position)
        own_length = jnp.where(inside, rows_here * band_total, own_length)
        offset_rows = offset_rows + rows_here
    return (own_position, own_length)


def draw_corners(key, part):
    band_total = TOKENS // BAND_ROWS
    own_position, own_length = query_place()
    tables = []
    for level_index in range(LEVELS):
        rows_here = ROWS_DEV // 4 ** level_index
        length = rows_here * band_total
        stride = MAP_W // 2 ** level_index
        shape_here = (TOKENS, HEADS, POINTS)
        keys_here = jax.random.split(jax.random.fold_in(key, 11 + level_index), 4)
        centre = (own_position * length // own_length)[:, None, None]
        jitter = jax.random.randint(keys_here[0], shape_here, -rows_here, rows_here + 1) + jax.random.randint(keys_here[1], shape_here, -rows_here, rows_here + 1)
        faraway = jax.random.randint(keys_here[2], shape_here, 0, length)
        choose = jax.random.randint(keys_here[3], shape_here, 0, 4) != 0
        anchor = jnp.clip(jnp.where(choose, faraway, centre + jitter), 0, length - stride - 2)
        tables.append(jnp.stack([anchor, anchor + 1, anchor + stride, anchor + stride + 1], axis=-1))
    return jnp.stack(tables, axis=2).reshape(TOKENS, HEADS * LEVELS * POINTS * 4).astype(jnp.int32)


def draw_bilinear(key, part):
    key_first, key_second = jax.random.split(jax.random.fold_in(key, 29))
    shape_here = (TOKENS, HEADS * LEVELS * POINTS)
    first = jax.random.uniform(key_first, shape_here, jnp.float32)
    second = jax.random.uniform(key_second, shape_here, jnp.float32)
    first = 0.3 + 0.4 * first
    second = 0.3 + 0.4 * second
    stacked = jnp.stack([(1.0 - first) * (1.0 - second), first * (1.0 - second), (1.0 - first) * second, first * second], axis=-1)
    return stacked.reshape(TOKENS, HEADS * LEVELS * POINTS * 4).astype(jnp.float32)


def draw_attention(key, part):
    key_logit = jax.random.fold_in(key, 37)
    shape_here = (TOKENS, HEADS, LEVELS * POINTS)
    finer = jnp.arange(LEVELS * POINTS, dtype=jnp.int32) // POINTS < 2
    noise = jax.random.normal(key_logit, shape_here, jnp.float32)
    logits = jnp.where(finer, 0.3 * noise, 1.35 + 0.8 * noise)
    return jax.nn.softmax(logits, axis=-1).reshape(TOKENS, HEADS * LEVELS * POINTS).astype(jnp.float32)


def block_scale(stream_key, shape, pieces, smallest, top_value):
    def one(axis_at, shards_of):
        steps = jax.random.uniform(jax.random.fold_in(jax.random.fold_in(stream_key, 6), axis_at), (shards_of,), jnp.float32, smallest / len(pieces), top_value / len(pieces))
        return jnp.repeat(jnp.exp(steps), shape[axis_at] // shards_of).reshape((-1,) + (1,) * (len(shape) - axis_at - 1))

    level = one(*pieces[0])
    for cut in pieces[1:]:
        level = level * one(*cut)
    return level


def bell_draw(rng, dims, deviation, limit, pieces=(), held_as=jnp.bfloat16):
    loudness = block_scale(rng, dims, pieces, -0.22, 0.18) if pieces else 1.0
    values = jax.random.normal(rng, dims, jnp.float32) * deviation * loudness
    return jnp.minimum(jnp.maximum(values, -limit), limit).astype(held_as)


def setup_inputs(seed: int = 0, part: int = 0) -> dict:
    key_list = jax.random.split(jax.random.key(seed), 17)
    own_keys = jax.random.split(jax.random.fold_in(key_list[16], part), 17)
    return {
        "features": bell_draw(own_keys[0], (TOKENS, D), 1.0, 6.0, ((0, 32),)),
        "corners": draw_corners(jax.random.fold_in(jax.random.fold_in(key_list[16], part), 71), part),
        "bilinear": draw_bilinear(jax.random.fold_in(jax.random.fold_in(key_list[16], part), 71), part),
        "attention": draw_attention(jax.random.fold_in(jax.random.fold_in(key_list[16], part), 71), part),
        "w_value": bell_draw(key_list[4], (D, D), D ** -0.5, 0.375),
        "b_value": bell_draw(key_list[5], (D,), 0.1, 0.6, (), jnp.float32),
        "w_out": bell_draw(key_list[6], (D, D), (D // 16) ** -0.5, 1.5),
        "b_out": bell_draw(key_list[7], (D,), 0.5, 3.0, (), jnp.float32),
        "norm1_gain": jnp.clip(1.0 + 0.1 * jax.random.normal(key_list[8], (D,), jnp.float32), 0.5, 1.5),
        "norm1_bias": bell_draw(key_list[9], (D,), 0.5, 3.0, (), jnp.float32),
        "w_in": bell_draw(key_list[10], (D, FF), D ** -0.5, 0.375),
        "b_in": bell_draw(key_list[11], (FF,), 0.5, 3.0, (), jnp.float32),
        "w_ffout": bell_draw(key_list[12], (FF, D), FF ** -0.5, 0.1875),
        "b_ffout": bell_draw(key_list[13], (D,), 0.5, 3.0, (), jnp.float32),
        "norm2_gain": jnp.clip(1.0 + 0.1 * jax.random.normal(key_list[14], (D,), jnp.float32), 0.5, 1.5),
        "norm2_bias": bell_draw(key_list[15], (D,), 0.5, 3.0, (), jnp.float32),
    }


def layer_norm(inputs, gain, shift):
    average = lax.optimization_barrier(jnp.mean(inputs, axis=-1, keepdims=True))
    centred = inputs - average
    variance = lax.optimization_barrier(jnp.mean(centred * centred, axis=-1, keepdims=True))
    return centred * lax.rsqrt(variance + 1e-05) * gain + shift

def reference(features, corners, bilinear, attention, w_value, b_value, w_out, b_out, norm1_gain, norm1_bias, w_in, b_in, w_ffout, b_ffout, norm2_gain, norm2_bias):
    token_count, model_width = features.shape
    head_dim = model_width // HEADS
    samples = LEVELS * POINTS * 4
    segment_rows = [ROWS_DEV // 4 ** level_index for level_index in range(LEVELS)]
    segment_start = [sum(segment_rows[:level_index]) for level_index in range(LEVELS)]
    value_rows = (jnp.dot(features, w_value, preferred_element_type=jnp.float32) + b_value).astype(jnp.bfloat16)
    weight = (attention.reshape(token_count, HEADS, LEVELS, POINTS, 1) * bilinear.reshape(token_count, HEADS, LEVELS, POINTS, 4)).astype(jnp.bfloat16)
    weight = weight.reshape(token_count, HEADS, samples)
    corner_table = corners.reshape(token_count, HEADS, LEVELS, POINTS * 4)
    places = []
    for level_index in range(LEVELS):
        level_corner = corner_table[:, :, level_index]
        places.append(level_corner // segment_rows[level_index] * BAND_ROWS + segment_start[level_index] + level_corner % segment_rows[level_index])
    place_table = jnp.stack(places, axis=2).reshape(token_count, HEADS, samples)
    flat_index = (place_table * HEADS + jnp.arange(HEADS, dtype=jnp.int32)[None, :, None]).astype(jnp.int32)
    flat_value = value_rows.reshape(token_count * HEADS, head_dim)
    band_count = token_count // BAND_ROWS

    def blend_block(block_args):
        index_block, weight_block = block_args
        picked = flat_value[index_block].astype(jnp.float32)
        return lax.optimization_barrier(jnp.sum(weight_block.astype(jnp.float32)[..., None] * picked, axis=2))
    sampled = lax.map(blend_block, (flat_index.reshape(band_count, BAND_ROWS, HEADS, samples), weight.reshape(band_count, BAND_ROWS, HEADS, samples)))
    sampled = sampled.reshape(token_count, model_width).astype(jnp.bfloat16)
    attended = jnp.dot(sampled, w_out, preferred_element_type=jnp.float32) + b_out
    middle = layer_norm(features.astype(jnp.float32) + attended, norm1_gain, norm1_bias).astype(jnp.bfloat16)
    hidden = jnp.maximum(jnp.dot(middle, w_in, preferred_element_type=jnp.float32) + b_in, 0.0).astype(jnp.bfloat16)
    result = middle.astype(jnp.float32) + jnp.dot(hidden, w_ffout, preferred_element_type=jnp.float32) + b_ffout
    return layer_norm(result, norm2_gain, norm2_bias).astype(jnp.bfloat16)
```

```python
import jax
import jax.numpy as jnp
from jax import lax
from jax.experimental import pallas as pl
from jax.experimental.pallas import tpu as pltpu
from jax.sharding import Mesh
from jax.sharding import PartitionSpec as P

MESH_ID = pl.DeviceIdType.MESH
DP_BAND = ("dp", "band_0", "band_1")
HEADS = 8
NY, NZ = 4, 8
BANDS = NY * NZ
BAND_ROWS = 255
PAD = 256
LEVEL_ROWS = (6144, 1536, 384, 96)
LEVEL_AT = (0, 6144, 7680, 8064)
STRIDE = (128, 64, 32, 16)
BAND_PART = (192, 48, 12, 3)
BAND_AT = (0, 192, 240, 252)
TOKENS = 8160
POINTS = 16
BF = jnp.bfloat16
F32 = jnp.float32
VM = pltpu.VMEM


def dot(a, b, ca, cb, precision=None):
    return lax.dot_general(
        a, b, (((ca,), (cb,)), ((), ())), preferred_element_type=F32, precision=precision
    )


def onehot(rows, columns, hit):
    r = lax.broadcasted_iota(jnp.int32, (rows, columns), 0)
    c = lax.broadcasted_iota(jnp.int32, (rows, columns), 1)
    return hit(r, c).astype(BF)


def exchange_kernel(
    feat, corner, bil, att, w_value, b_value, table, index, weight,
    send_v, send_i, send_w, sems_out, sems_in, y_out, y_in,
):
    y = lax.axis_index("band_0")
    z = lax.axis_index("band_1")
    barrier = pltpu.get_barrier_semaphore()
    for d in range(1, NZ):
        pl.semaphore_signal(
            barrier, inc=1, device_id={"band_1": lax.rem(z + d, NZ)}, device_id_type=MESH_ID
        )
    for d in range(1, NY):
        pl.semaphore_signal(
            barrier, inc=1, device_id={"band_0": lax.rem(y + d, NY)}, device_id_type=MESH_ID
        )

    values = (dot(feat[...], w_value[...], 1, 0) + b_value[...]).astype(BF)
    eye = onehot(256, 256, lambda r, c: r == c)
    turned = dot(eye, values, 1, 1).astype(BF)
    send_v[:, :, 0:BAND_ROWS] = turned.reshape(HEADS, 32, BAND_ROWS)
    pl.semaphore_wait(barrier, NZ + NY - 2)

    here = y * NZ + z

    def z_copy(kind, src, dst, d):
        t = lax.rem(z + d, NZ)
        slot = here if kind == 0 else z
        return pltpu.make_async_remote_copy(
            src_ref=src.at[t],
            dst_ref=dst.at[slot],
            send_sem=sems_out.at[kind, d],
            recv_sem=sems_in.at[kind, d],
            device_id={"band_1": t},
            device_id_type=MESH_ID,
        )

    v_copies = [z_copy(0, send_v, table, d) for d in range(1, NZ)]
    for c in v_copies:
        c.start()
    table[here] = send_v[z]

    pick = onehot(128, 512, lambda r, c: c == 4 * r)
    ids = corner[...]
    high = (ids // 64).astype(F32).astype(BF)
    low = (ids % 64).astype(F32).astype(BF)
    anchor = (dot(pick, high, 1, 1) * 64.0 + dot(pick, low, 1, 1)).astype(jnp.int32)
    level = (lax.broadcasted_iota(jnp.int32, (128, BAND_ROWS), 0) // 4) % 4
    base = jnp.where(
        level == 0,
        LEVEL_AT[0],
        jnp.where(level == 1, LEVEL_AT[1], jnp.where(level == 2, LEVEL_AT[2], LEVEL_AT[3])),
    )
    send_i[...] = jnp.zeros((HEADS, POINTS, PAD), jnp.int32)
    send_i[:, :, 0:BAND_ROWS] = (anchor + base).reshape(HEADS, POINTS, BAND_ROWS)
    i_copies = [z_copy(1, send_i, index, d) for d in range(1, NZ)]
    for c in i_copies:
        c.start()
    index[z] = send_i[z]

    spread = onehot(128, 512, lambda r, c: c // 4 == r).astype(F32)
    each = dot(att[...], spread, 1, 0, lax.Precision.HIGHEST)
    product = (each * bil[...]).astype(BF)
    eye2 = onehot(512, 512, lambda r, c: r == c)
    send_w[:, :, 0:BAND_ROWS] = dot(eye2, product, 1, 1).astype(BF).reshape(HEADS, 64, BAND_ROWS)
    w_copies = [z_copy(2, send_w, weight, d) for d in range(1, NZ)]
    for c in w_copies:
        c.start()
    weight[z] = send_w[z]

    for c in v_copies:
        c.wait_recv()
    y_copies = []
    part = table.at[pl.ds(y * NZ, NZ)]
    for d in range(1, NY):
        y_copies.append(
            pltpu.make_async_remote_copy(
                src_ref=part,
                dst_ref=part,
                send_sem=y_out.at[d],
                recv_sem=y_in.at[d],
                device_id={"band_0": lax.rem(y + d, NY)},
                device_id_type=MESH_ID,
            )
        )
    for c in y_copies:
        c.start()
    for c in i_copies + w_copies:
        c.wait_recv()
    for c in y_copies:
        c.wait_recv()
    for c in v_copies + i_copies + w_copies + y_copies:
        c.wait_send()


def exchange(feat, corner, bil, att, w_value, b_value):
    sem = pltpu.SemaphoreType.DMA
    return pl.pallas_call(
        exchange_kernel,
        out_shape=(
            jax.ShapeDtypeStruct((BANDS, 32, PAD), BF),
            jax.ShapeDtypeStruct((HEADS, POINTS, PAD), jnp.int32),
            jax.ShapeDtypeStruct((HEADS, 64, PAD), BF),
        ),
        in_specs=[pl.BlockSpec(memory_space=VM)] * 6,
        out_specs=(pl.BlockSpec(memory_space=VM),) * 3,
        scratch_shapes=[
            VM((HEADS, 32, PAD), BF),
            VM((HEADS, POINTS, PAD), jnp.int32),
            VM((HEADS, 64, PAD), BF),
            sem((3, NZ)),
            sem((3, NZ)),
            sem((NY,)),
            sem((NY,)),
        ],
        compiler_params=pltpu.CompilerParams(collective_id=0, has_side_effects=True),
        name="exchange",
    )(feat, corner, bil, att, w_value, b_value)


def build_table(parts, rows, table):
    rep = onehot(32, 128, lambda r, c: c % 32 == r)
    rows[TOKENS : TOKENS + 160, :] = jnp.zeros((160, 128), F32)
    for b in range(BANDS):
        wide = dot(parts[b], rep, 0, 0)
        for at, part, first in zip(LEVEL_AT, BAND_PART, BAND_AT):
            rows[at + b * part : at + (b + 1) * part, :] = wide[first : first + part, :]
    for at, count, stride in zip(LEVEL_AT, LEVEL_ROWS, STRIDE):
        size = min(count, 128)
        lane = lax.broadcasted_iota(jnp.int32, (size, 128), 1)

        def step(i, carry, at=at, size=size, stride=stride, lane=lane):
            k = pl.multiple_of(at + i * size, 8)
            first = rows[pl.ds(k, size), :]
            second = rows[pl.ds(k + 1, size), :]
            third = rows[pl.ds(pl.multiple_of(k + stride, 8), size), :]
            fourth = rows[pl.ds(k + stride + 1, size), :]
            table[pl.ds(k, size), :] = jnp.where(
                lane < 64, jnp.where(lane < 32, first, second), jnp.where(lane < 96, third, fourth)
            )
            return carry

        lax.fori_loop(0, count // size, step, 0)


def blend_kernel(index, weight, parts, out, rows, table, picked, spread, ids, sem):
    def fetch(j):
        return pltpu.make_async_copy(index.at[j], ids, sem)

    fetch(0).start()
    build_table(parts, rows, table)
    widen = onehot(64, POINTS * 128, lambda r, c: c // 32 == r)
    rep = onehot(32, 128, lambda r, c: c % 32 == r)

    def block(j, carry):
        fetch(j).wait()
        spread[...] = dot(weight[j], widen, 0, 0)
        for p in range(POINTS):
            for q in range(PAD):
                picked[p * PAD + q : p * PAD + q + 1, :] = table[pl.ds(ids[p, q], 1), :]

        @pl.when(j < HEADS - 1)
        def _():
            fetch(j + 1).start()

        total = picked[0:PAD, :] * spread[:, 0:128]
        for p in range(1, POINTS):
            total += picked[p * PAD : (p + 1) * PAD, :] * spread[:, p * 128 : (p + 1) * 128]
        major = total.astype(BF)
        minor = (total - major.astype(F32)).astype(BF)
        out[j] = (dot(rep, major, 1, 1) + dot(rep, minor, 1, 1)).astype(BF)
        return carry

    lax.fori_loop(0, HEADS, block, 0)


def blend(index, weight, parts):
    return pl.pallas_call(
        blend_kernel,
        out_shape=jax.ShapeDtypeStruct((HEADS, 32, PAD), BF),
        in_specs=[pl.BlockSpec(memory_space=VM)] * 3,
        out_specs=pl.BlockSpec(memory_space=VM),
        scratch_shapes=[
            VM((TOKENS + 160, 128), F32),
            VM((TOKENS, 128), F32),
            VM((POINTS * PAD, 128), F32),
            VM((PAD, POINTS * 128), F32),
            pltpu.SMEM((POINTS, PAD), jnp.int32),
            pltpu.SemaphoreType.DMA,
        ],
        compiler_params=pltpu.CompilerParams(vmem_limit_bytes=56 << 20),
        name="blend",
    )(index, weight, parts)


def layer_norm(inputs, gain, shift):
    average = jnp.mean(inputs, axis=-1, keepdims=True)
    centred = inputs - average
    variance = jnp.mean(centred * centred, axis=-1, keepdims=True)
    return centred * lax.rsqrt(variance + 1e-05) * gain + shift


def finish_kernel(
    blended, feat, w_out, b_out, gain1, shift1, w_in, b_in, w_ff, b_ff, gain2, shift2,
    out, heads, sem_out, sem_in,
):
    z = lax.axis_index("band_1")
    barrier = pltpu.get_barrier_semaphore()
    for d in range(1, NZ):
        pl.semaphore_signal(
            barrier, inc=1, device_id={"band_1": lax.rem(z + d, NZ)}, device_id_type=MESH_ID
        )
    pl.semaphore_wait(barrier, NZ - 1)
    copies = []
    for d in range(1, NZ):
        t = lax.rem(z + d, NZ)
        copies.append(
            pltpu.make_async_remote_copy(
                src_ref=blended.at[t],
                dst_ref=heads.at[z],
                send_sem=sem_out.at[d],
                recv_sem=sem_in.at[d],
                device_id={"band_1": t},
                device_id_type=MESH_ID,
            )
        )
    for c in copies:
        c.start()
    heads[z] = blended[z]
    for c in copies:
        c.wait_recv()
    sampled = heads[...].reshape(256, PAD)
    attended = dot(sampled, w_out[...], 0, 0)[0:BAND_ROWS] + b_out[...]
    middle = layer_norm(feat[...].astype(F32) + attended, gain1[...], shift1[...]).astype(BF)
    hidden = jnp.maximum(dot(middle, w_in[...], 1, 0) + b_in[...], 0.0).astype(BF)
    result = middle.astype(F32) + dot(hidden, w_ff[...], 1, 0) + b_ff[...]
    out[...] = layer_norm(result, gain2[...], shift2[...]).astype(BF)
    for c in copies:
        c.wait_send()


def finish(blended, feat, *params):
    return pl.pallas_call(
        finish_kernel,
        out_shape=jax.ShapeDtypeStruct((BAND_ROWS, 256), BF),
        in_specs=[pl.BlockSpec(memory_space=VM)] * 12,
        out_specs=pl.BlockSpec(memory_space=VM),
        scratch_shapes=[
            VM((HEADS, 32, PAD), BF),
            pltpu.SemaphoreType.DMA((NZ,)),
            pltpu.SemaphoreType.DMA((NZ,)),
        ],
        compiler_params=pltpu.CompilerParams(collective_id=1, has_side_effects=True),
        name="finish",
    )(blended, feat, *params)


def body(
    features, corners, bilinear, attention, w_value, b_value, w_out, b_out,
    norm1_gain, norm1_bias, w_in, b_in, w_ffout, b_ffout, norm2_gain, norm2_bias,
):
    def row(x):
        return x.reshape(1, -1)

    parts, index, weight = exchange(
        features, corners, bilinear, attention, w_value, row(b_value)
    )
    blended = blend(index, weight, parts)
    return finish(
        blended, features, w_out, row(b_out), row(norm1_gain), row(norm1_bias), w_in, row(b_in),
        w_ffout, row(b_ffout), row(norm2_gain), row(norm2_bias),
    )


def solution(mesh):
    split = Mesh(mesh.devices.reshape(mesh.shape["dp"], NY, NZ), DP_BAND)
    return jax.shard_map(
        body,
        mesh=split,
        in_specs=(P(DP_BAND, None),) * 4 + (P(),) * 12,
        out_specs=P(DP_BAND, None),
        check_vma=False,
    )
```

```python
import jax
import jax.numpy as jnp
from jax import lax
from jax.experimental import pallas as pl
from jax.experimental.pallas import tpu as pltpu
from jax.sharding import Mesh
from jax.sharding import PartitionSpec as P

MESH_ID = pl.DeviceIdType.MESH
DP_BAND = ("dp", "band_0", "band_1")
HEADS = 8
NY, NZ = 4, 8
BANDS = NY * NZ
BAND_ROWS = 255
PAD = 256
LEVEL_ROWS = (6144, 1536, 384, 96)
LEVEL_AT = (0, 6144, 7680, 8064)
STRIDE = (128, 64, 32, 16)
BAND_PART = (192, 48, 12, 3)
BAND_AT = (0, 192, 240, 252)
TOKENS = 8160
POINTS = 16
BF = jnp.bfloat16
F32 = jnp.float32
VM = pltpu.VMEM


def dot(a, b, ca, cb, precision=None):
    return lax.dot_general(
        a, b, (((ca,), (cb,)), ((), ())), preferred_element_type=F32, precision=precision
    )


def onehot(rows, columns, hit):
    r = lax.broadcasted_iota(jnp.int32, (rows, columns), 0)
    c = lax.broadcasted_iota(jnp.int32, (rows, columns), 1)
    return hit(r, c).astype(BF)


def layer_norm(inputs, gain, shift):
    average = jnp.mean(inputs, axis=-1, keepdims=True)
    centred = inputs - average
    variance = jnp.mean(centred * centred, axis=-1, keepdims=True)
    return centred * lax.rsqrt(variance + 1e-05) * gain + shift


def layer_kernel(
    feat_in, corner_in, bil_in, att_in, w_value_in, b_value, w_out_in, b_out, gain1, shift1,
    w_in_in, b_in, w_ff_in, b_ff, gain2, shift2,
    out,
    feat, corner, bil, att, w_value, w_out, w_in, w_ff, turned_ids,
    send_v, send_i, send_w, parts, index, weight,
    rows, table, small, picked_a, picked_b, spread_a, spread_b, side_a, side_b, lanes_a, lanes_b,
    major, minor, done, heads, ids_a, ids_b,
    load_sem, ids_sem, sems_out, sems_in, y_out, y_in,
):
    y = lax.axis_index("band_0")
    z = lax.axis_index("band_1")
    here = y * NZ + z
    barrier = pltpu.get_barrier_semaphore()
    for d in range(1, NZ):
        pl.semaphore_signal(
            barrier, inc=1, device_id={"band_1": lax.rem(z + d, NZ)}, device_id_type=MESH_ID
        )
    for d in range(1, NY):
        pl.semaphore_signal(
            barrier, inc=1, device_id={"band_0": lax.rem(y + d, NY)}, device_id_type=MESH_ID
        )
    loads = [
        pltpu.make_async_copy(src, dst, load_sem.at[i])
        for i, (src, dst) in enumerate(
            (
                (feat_in, feat), (w_value_in, w_value), (corner_in, corner), (att_in, att),
                (bil_in, bil), (w_out_in, w_out), (w_in_in, w_in), (w_ff_in, w_ff),
            )
        )
    ]
    for c in loads:
        c.start()

    def z_copy(kind, src, dst, slot, d, back=False):
        t = lax.rem(z + NZ - d, NZ) if back else lax.rem(z + d, NZ)
        return pltpu.make_async_remote_copy(
            src_ref=src.at[t],
            dst_ref=dst.at[slot],
            send_sem=sems_out.at[kind, d],
            recv_sem=sems_in.at[kind, d],
            device_id={"band_1": t},
            device_id_type=MESH_ID,
        )

    def v_copy(d):
        return z_copy(0, send_v, parts, here, d)

    def i_copy(d):
        return z_copy(1, send_i, index, z, d)

    def w_copy(d):
        return z_copy(2, send_w, weight, z, d)

    def h_copy(d):
        return z_copy(3, done, heads, z, d, back=True)

    loads[0].wait()
    loads[1].wait()
    values = (dot(feat[...], w_value[...], 1, 0) + b_value[...]).astype(BF)
    eye = onehot(256, 256, lambda r, c: r == c)
    turned = dot(eye, values, 1, 1).astype(BF)
    send_v[:, :, 0:BAND_ROWS] = turned.reshape(HEADS, 32, BAND_ROWS)
    pl.semaphore_wait(barrier, NZ + NY - 2)
    for d in range(1, NZ):
        v_copy(d).start()
    parts[here] = send_v[z]

    loads[2].wait()
    turned_ids[0, :, :] = jnp.transpose(corner[0:128, :])
    turned_ids[1, :, 0 : BAND_ROWS - 128] = jnp.transpose(corner[128:BAND_ROWS, :])
    level = (lax.broadcasted_iota(jnp.int32, (128, 128), 0) // 4) % 4
    base = jnp.where(
        level == 0,
        LEVEL_AT[0],
        jnp.where(level == 1, LEVEL_AT[1], jnp.where(level == 2, LEVEL_AT[2], LEVEL_AT[3])),
    )
    used = lax.broadcasted_iota(jnp.int32, (128, 128), 1) < BAND_ROWS - 128
    left = turned_ids[0, pl.ds(0, 128, stride=4), :] + base
    right = jnp.where(used, turned_ids[1, pl.ds(0, 128, stride=4), :] + base, 0)
    send_i[:, :, 0:128] = left.reshape(HEADS, POINTS, 128)
    send_i[:, :, 128:256] = right.reshape(HEADS, POINTS, 128)
    for d in range(1, NZ):
        i_copy(d).start()
    index[z] = send_i[z]

    loads[3].wait()
    loads[4].wait()
    repeat = onehot(128, 512, lambda r, c: c // 4 == r)
    whole = att[...]
    first = whole.astype(BF)
    rest = whole - first.astype(F32)
    second = rest.astype(BF)
    third = (rest - second.astype(F32)).astype(BF)
    each = dot(first, repeat, 1, 0) + dot(second, repeat, 1, 0) + dot(third, repeat, 1, 0)
    product = (each * bil[...]).astype(BF)
    eye2 = onehot(512, 512, lambda r, c: r == c)
    send_w[:, :, 0:BAND_ROWS] = dot(eye2, product, 1, 1).astype(BF).reshape(HEADS, 64, BAND_ROWS)
    for d in range(1, NZ):
        w_copy(d).start()
    weight[z] = send_w[z]

    for d in range(1, NZ):
        v_copy(d).wait_recv()
    part = parts.at[pl.ds(y * NZ, NZ)]
    y_copies = [
        pltpu.make_async_remote_copy(
            src_ref=part,
            dst_ref=part,
            send_sem=y_out.at[d],
            recv_sem=y_in.at[d],
            device_id={"band_0": lax.rem(y + d, NY)},
            device_id_type=MESH_ID,
        )
        for d in range(1, NY)
    ]
    for c in y_copies:
        c.start()
    for c in y_copies:
        c.wait_recv()

    rows[TOKENS : TOKENS + 160, :] = jnp.zeros((160, 128), F32)
    rep = onehot(32, 128, lambda r, c: c % 32 == r)
    for b in range(BANDS):
        wide = dot(parts[b], rep, 0, 0)
        for at, count, begin in zip(LEVEL_AT, BAND_PART, BAND_AT):
            rows[at + b * count : at + (b + 1) * count, :] = wide[begin : begin + count, :]
    for at, count, stride in zip(LEVEL_AT[:2], LEVEL_ROWS[:2], STRIDE[:2]):
        lane = lax.broadcasted_iota(jnp.int32, (128, 128), 1)

        def four(i, carry, at=at, stride=stride, lane=lane):
            k = pl.multiple_of(at + i * 128, 8)
            c0 = rows[pl.ds(k, 128), :]
            c1 = rows[pl.ds(k + 1, 128), :]
            c2 = rows[pl.ds(pl.multiple_of(k + stride, 8), 128), :]
            c3 = rows[pl.ds(k + stride + 1, 128), :]
            table[pl.ds(k, 128), :] = jnp.where(
                lane < 64, jnp.where(lane < 32, c0, c1), jnp.where(lane < 96, c2, c3)
            )
            return carry

        lax.fori_loop(0, count // 128, four, 0)
    pick = onehot(32, 128, lambda r, c: r == c)
    small[...] = dot(pick, rows[LEVEL_AT[2] : LEVEL_AT[2] + 512, :].astype(BF), 1, 1)

    widen = onehot(32, 8 * 128, lambda r, c: c // 32 == r)
    set_a = (picked_a, spread_a, side_a, lanes_a, ids_a, 0)
    set_b = (picked_b, spread_b, side_b, lanes_b, ids_b, 1)

    def owner(d):
        return lax.rem(z + NZ - d, NZ)

    def fetch(d, bufs):
        return pltpu.make_async_copy(
            index.at[owner(d), pl.ds(0, 8)], bufs[4], ids_sem.at[bufs[5]]
        )

    def lanes_part(j, side, lanes, r):
        half, i = r % 2, r // 2
        at = slice(half * 128, half * 128 + 128)
        sums = [lanes[v * 8 : v * 8 + 8, at] for v in range(4)]
        for point, level in ((i, 2), (i + 4, 3)):
            place = index[j, 8 + point : 9 + point, at] - LEVEL_AT[2]
            for c, off in enumerate((0, 1, STRIDE[level], STRIDE[level] + 1)):
                spot = jnp.broadcast_to(place + off, (8, 128))
                lane = spot & 127
                group = spot >> 7
                w = jnp.broadcast_to(side[point * 4 + c : point * 4 + c + 1, at], (8, 128))
                for v in range(4):

                    def take(g):
                        window = small[v * 8 : v * 8 + 8, g * 128 : g * 128 + 128]
                        return jnp.take_along_axis(
                            window, lane, axis=1, mode="promise_in_bounds"
                        )

                    if level == 3:
                        got = take(3)
                    else:
                        got = jnp.where(
                            group == 0, take(0), jnp.where(group == 1, take(1), take(2))
                        )
                    sums[v] = sums[v] + got * w
        for v in range(4):
            lanes[v * 8 : v * 8 + 8, at] = sums[v]

    def add_up(bufs, c):
        picked, spread = bufs[0], bufs[1]
        total = None
        for r in range(8):
            term = (
                picked[r * PAD + c * 32 : r * PAD + c * 32 + 32, :]
                * spread[c * 32 : c * 32 + 32, r * 128 : r * 128 + 128]
            )
            total = term if total is None else total + term
        top = total.astype(BF)
        major[c * 32 : c * 32 + 32, :] = top
        minor[c * 32 : c * 32 + 32, :] = (total - top.astype(F32)).astype(BF)

    def close(d, bufs):
        done[owner(d)] = (
            dot(rep, major[...], 1, 1) + dot(rep, minor[...], 1, 1) + bufs[3][...]
        ).astype(BF)

    def send_back(d):
        @pl.when(d == 0)
        def _():
            heads[z] = done[z]

        @pl.when(d > 0)
        def _():
            h_copy(d).start()

    def stage(d, bufs, other, last):
        picked, spread, side, lanes, ids, _ = bufs
        j = owner(d)
        if not last:
            i_copy(d + 1).wait_recv()
            fetch(d + 1, other).start()
        else:

            @pl.when(d < NZ - 1)
            def _():
                i_copy(d + 1).wait_recv()
                fetch(d + 1, other).start()

        @pl.when(d > 0)
        def _():
            w_copy(d).wait_recv()

        fetch(d, bufs).wait()
        spread[...] = dot(weight[j, 0:32, :], widen, 0, 0)
        side[...] = weight[j, 32:64, :].astype(F32)
        lanes[...] = jnp.zeros((32, PAD), F32)
        for r in range(8):

            @pl.when(d > -1 - r)
            def _(r=r):
                for q in range(PAD):
                    picked[r * PAD + q : r * PAD + q + 1, :] = table[pl.ds(ids[r, q], 1), :]
                lanes_part(j, side, lanes, r)
                add_up(other, r)

    fetch(0, set_a).start()

    def pair(i, carry):
        d = 2 * i
        stage(d, set_a, set_b, False)

        @pl.when(i > 0)
        def _():
            close(d - 1, set_b)
            send_back(d - 1)

        stage(d + 1, set_b, set_a, True)
        close(d, set_a)
        send_back(d)
        return carry

    lax.fori_loop(0, NZ // 2, pair, 0)
    for c in range(8):
        add_up(set_b, c)
    close(NZ - 1, set_b)
    send_back(NZ - 1)

    for c in loads[5:]:
        c.wait()
    for d in range(1, NZ):
        h_copy(d).wait_recv()
    sampled = heads[...].reshape(256, PAD)
    attended = dot(sampled, w_out[...], 0, 0)[0:BAND_ROWS] + b_out[...]
    middle = layer_norm(feat[...].astype(F32) + attended, gain1[...], shift1[...]).astype(BF)
    hidden = jnp.maximum(dot(middle, w_in[...], 1, 0) + b_in[...], 0.0).astype(BF)
    result = middle.astype(F32) + dot(hidden, w_ff[...], 1, 0) + b_ff[...]
    out[...] = layer_norm(result, gain2[...], shift2[...]).astype(BF)
    for d in range(1, NZ):
        for c in (v_copy(d), i_copy(d), w_copy(d), h_copy(d)):
            c.wait_send()
    for c in y_copies:
        c.wait_send()


def body(
    features, corners, bilinear, attention, w_value, b_value, w_out, b_out,
    norm1_gain, norm1_bias, w_in, b_in, w_ffout, b_ffout, norm2_gain, norm2_bias,
):
    def row(x):
        return x.reshape(1, -1)

    def like(x):
        return VM(x.shape, x.dtype)

    dma = pltpu.SemaphoreType.DMA
    big = pl.BlockSpec(memory_space=pl.ANY)
    vec = pl.BlockSpec(memory_space=VM)
    return pl.pallas_call(
        layer_kernel,
        out_shape=jax.ShapeDtypeStruct((BAND_ROWS, 256), BF),
        in_specs=[big] * 5 + [vec, big, vec, vec, vec, big, vec, big, vec, vec, vec],
        out_specs=vec,
        scratch_shapes=[
            like(features), like(corners), like(bilinear), like(attention), like(w_value),
            like(w_out), like(w_in), like(w_ffout),
            VM((2, 512, 128), jnp.int32),
            VM((HEADS, 32, PAD), BF),
            VM((HEADS, POINTS, PAD), jnp.int32),
            VM((HEADS, 64, PAD), BF),
            VM((BANDS, 32, PAD), BF),
            VM((HEADS, POINTS, PAD), jnp.int32),
            VM((HEADS, 64, PAD), BF),
            VM((TOKENS + 160, 128), F32),
            VM((LEVEL_AT[2], 128), F32),
            VM((32, 512), F32),
            VM((8 * PAD, 128), F32),
            VM((8 * PAD, 128), F32),
            VM((PAD, 8 * 128), F32),
            VM((PAD, 8 * 128), F32),
            VM((32, PAD), F32),
            VM((32, PAD), F32),
            VM((32, PAD), F32),
            VM((32, PAD), F32),
            VM((PAD, 128), BF),
            VM((PAD, 128), BF),
            VM((HEADS, 32, PAD), BF),
            VM((HEADS, 32, PAD), BF),
            pltpu.SMEM((8, PAD), jnp.int32),
            pltpu.SMEM((8, PAD), jnp.int32),
            dma((8,)),
            dma((2,)),
            dma((4, NZ)),
            dma((4, NZ)),
            dma((NY,)),
            dma((NY,)),
        ],
        compiler_params=pltpu.CompilerParams(
            collective_id=0, has_side_effects=True, vmem_limit_bytes=60 << 20
        ),
        name="layer",
    )(
        features, corners, bilinear, attention, w_value, row(b_value), w_out, row(b_out),
        row(norm1_gain), row(norm1_bias), w_in, row(b_in), w_ffout, row(b_ffout),
        row(norm2_gain), row(norm2_bias),
    )


def solution(mesh):
    split = Mesh(mesh.devices.reshape(mesh.shape["dp"], NY, NZ), DP_BAND)
    return jax.shard_map(
        body,
        mesh=split,
        in_specs=(P(DP_BAND, None),) * 4 + (P(),) * 12,
        out_specs=P(DP_BAND, None),
        check_vma=False,
    )
```

```python
import jax
import jax.numpy as jnp
from jax import lax
from jax.experimental import pallas as pl
from jax.experimental.pallas import tpu as pltpu
from jax.sharding import Mesh
from jax.sharding import PartitionSpec as P

MESH_ID = pl.DeviceIdType.MESH
DP_BAND = ("dp", "band_0", "band_1")
HEADS = 8
NY, NZ = 4, 8
BANDS = NY * NZ
BAND_ROWS = 255
PAD = 256
LEVEL_ROWS = (6144, 1536, 384, 96)
LEVEL_AT = (0, 6144, 7680, 8064)
STRIDE = (128, 64, 32, 16)
BAND_PART = (192, 48, 12, 3)
BAND_AT = (0, 192, 240, 252)
TOKENS = 8160
POINTS = 16
BF = jnp.bfloat16
F32 = jnp.float32
VM = pltpu.VMEM


def dot(a, b, ca, cb, precision=None):
    return lax.dot_general(
        a, b, (((ca,), (cb,)), ((), ())), preferred_element_type=F32, precision=precision
    )


def onehot(rows, columns, hit):
    r = lax.broadcasted_iota(jnp.int32, (rows, columns), 0)
    c = lax.broadcasted_iota(jnp.int32, (rows, columns), 1)
    return hit(r, c).astype(BF)


def layer_norm(inputs, gain, shift):
    average = jnp.mean(inputs, axis=-1, keepdims=True)
    centred = inputs - average
    variance = jnp.mean(centred * centred, axis=-1, keepdims=True)
    return centred * lax.rsqrt(variance + 1e-05) * gain + shift


def layer_kernel(
    feat_in, corner_in, bil_in, att_in, w_value_in, b_value_in, w_out_in, b_out_in, gain1_in, shift1_in,
    w_in_in, b_in_in, w_ff_in, b_ff_in, gain2_in, shift2_in,
    out,
    feat, corner, bil, att, w_value, b_value, w_out, b_out, gain1, shift1, w_in, b_in, w_ff, b_ff,
    gain2, shift2, turned_ids,
    send_v, send_s, send_i, send_w, parts, smalls, index, weight, near_i, near_w, near_sum, coarse,
    rows, table, spread_a, spread_b, major_a, major_b, minor_a, minor_b, done, heads, ids_a, ids_b,
    load_sem, ids_sem, sems_out, sems_in, y_out, y_in,
):
    y = lax.axis_index("band_0")
    z = lax.axis_index("band_1")
    here = y * NZ + z
    barrier = pltpu.get_barrier_semaphore()
    for d in range(1, NZ):
        pl.semaphore_signal(
            barrier, inc=1, device_id={"band_1": lax.rem(z + d, NZ)}, device_id_type=MESH_ID
        )
    for d in (1, NY - 1):
        pl.semaphore_signal(
            barrier, inc=1, device_id={"band_0": lax.rem(y + d, NY)}, device_id_type=MESH_ID
        )
    loads = [
        pltpu.make_async_copy(src, dst, load_sem.at[i])
        for i, (src, dst) in enumerate(
            (
                (feat_in, feat), (w_value_in, w_value), (b_value_in, b_value), (corner_in, corner),
                (att_in, att), (bil_in, bil), (w_out_in, w_out), (b_out_in, b_out),
                (gain1_in, gain1), (shift1_in, shift1), (w_in_in, w_in), (b_in_in, b_in),
                (w_ff_in, w_ff), (b_ff_in, b_ff), (gain2_in, gain2), (shift2_in, shift2),
            )
        )
    ]
    for c in loads[0:3]:
        c.start()

    def z_copy(kind, src, dst, slot, d, back=False):
        t = lax.rem(z + NZ - d, NZ) if back else lax.rem(z + d, NZ)
        return pltpu.make_async_remote_copy(
            src_ref=src if src is send_s else src.at[t],
            dst_ref=dst.at[slot],
            send_sem=sems_out.at[kind, d],
            recv_sem=sems_in.at[kind, d],
            device_id={"band_1": t},
            device_id_type=MESH_ID,
        )

    def v_copy(d):
        return z_copy(0, send_v, parts, here, d)

    def i_copy(d):
        return z_copy(1, send_i, index, z, d)

    def w_copy(d):
        return z_copy(2, send_w, weight, z, d)

    def h_copy(d):
        return z_copy(3, done, heads, z, d, back=True)

    def s_copy(d):
        return z_copy(4, send_s, smalls, here, d)

    def y_copy(kind, ref, leg):
        step = (1, 1, NY - 1, NY - 1, 1, NY - 1)[leg]
        column = (y, y, y, y, lax.rem(y + NY - 1, NY), lax.rem(y + 1, NY))[leg]
        half = (0, 1, 1, 0, 0, 1)[leg]
        piece = ref.at[pl.ds(column * NZ + half * (NZ // 2), NZ // 2)]
        return pltpu.make_async_remote_copy(
            src_ref=piece,
            dst_ref=piece,
            send_sem=y_out.at[kind, leg],
            recv_sem=y_in.at[kind, leg],
            device_id={"band_0": lax.rem(y + step, NY)},
            device_id_type=MESH_ID,
        )

    for c in loads[0:3]:
        c.wait()
    for c in loads[3:]:
        c.start()
    values = (dot(feat[...], w_value[...], 1, 0) + b_value[...]).astype(BF)
    eye = onehot(256, 256, lambda r, c: r == c)
    turned = dot(eye, values, 1, 1).astype(BF)
    send_s[...] = jnp.zeros((16, 256), BF)
    send_s[0:15, :] = values[BAND_AT[2] : BAND_ROWS, :]
    send_v[:, :, 0:BAND_ROWS] = turned.reshape(HEADS, 32, BAND_ROWS)
    pl.semaphore_wait(barrier, NZ + 1)
    for d in range(1, NZ):
        s_copy(d).start()
    for d in range(1, NZ):
        v_copy(d).start()
    parts[here] = send_v[z]
    smalls[here] = send_s[...]

    loads[3].wait()
    turned_ids[0, :, :] = jnp.transpose(corner[0:128, :])
    turned_ids[1, :, 0 : BAND_ROWS - 128] = jnp.transpose(corner[128:BAND_ROWS, :])
    level = (lax.broadcasted_iota(jnp.int32, (128, 128), 0) // 4) % 4
    base = jnp.where(
        level == 0, LEVEL_AT[0], jnp.where(level == 1, LEVEL_AT[1], jnp.where(level == 2, 0, 384))
    )
    used = lax.broadcasted_iota(jnp.int32, (128, 128), 1) < BAND_ROWS - 128
    left = turned_ids[0, pl.ds(0, 128, stride=4), :] + base
    right = jnp.where(used, turned_ids[1, pl.ds(0, 128, stride=4), :] + base, 0)
    for at, side in ((0, left), (128, right)):
        side = side.reshape(HEADS, POINTS, 128)
        send_i[:, :, at : at + 128] = side[:, 0:8]
        near_i[:, :, at : at + 128] = side[:, 8:16]
    for d in range(1, NZ):
        i_copy(d).start()
    index[z] = send_i[z]

    loads[4].wait()
    loads[5].wait()
    repeat = onehot(128, 512, lambda r, c: c // 4 == r)
    whole = att[...]
    first = whole.astype(BF)
    rest = whole - first.astype(F32)
    second = rest.astype(BF)
    third = (rest - second.astype(F32)).astype(BF)
    each = dot(first, repeat, 1, 0) + dot(second, repeat, 1, 0) + dot(third, repeat, 1, 0)
    product = (each * bil[...]).astype(BF)
    eye2 = onehot(512, 512, lambda r, c: r == c)
    turned_w = dot(eye2, product, 1, 1).reshape(HEADS, 64, BAND_ROWS)
    send_w[:, :, 0:BAND_ROWS] = turned_w[:, 0:32].astype(BF)
    near_w[:, :, 0:BAND_ROWS] = turned_w[:, 32:64]
    for d in range(1, NZ):
        w_copy(d).start()
    weight[z] = send_w[z]

    widen = onehot(32, 8 * 128, lambda r, c: c // 32 == r)
    sub = lax.broadcasted_iota(jnp.int32, (8, 128), 0)
    set_a = (spread_a, major_a, minor_a, ids_a, 0)
    set_b = (spread_b, major_b, minor_b, ids_b, 1)

    def owner(d):
        return lax.rem(z + 2 * NZ - d, NZ)

    def fetch(d, bufs):
        return pltpu.make_async_copy(index.at[owner(d)], bufs[3], ids_sem.at[bufs[4]])

    spread_a[...] = dot(weight[z], widen, 0, 0)
    major_b[...] = jnp.zeros((PAD, 128), BF)
    minor_b[...] = jnp.zeros((PAD, 128), BF)
    fetch(0, set_a).start()

    for d in range(1, NZ):
        s_copy(d).wait_recv()
    for leg in range(4):
        y_copy(1, smalls, leg).start()
    rep = onehot(32, 128, lambda r, c: c % 32 == r)
    for d in range(1, NZ):
        v_copy(d).wait_recv()
    for leg in (0, 2):
        y_copy(0, parts, leg).start()

    def add_rows(column):
        for i in range(NZ):
            b = column * NZ + i
            wide = dot(parts[b], rep, 0, 0)
            for at, count, begin in zip(LEVEL_AT[:2], BAND_PART[:2], BAND_AT[:2]):
                rows[pl.ds(pl.multiple_of(at + b * count, 16), count), :] = wide[
                    begin : begin + count, :
                ]

    rows[LEVEL_AT[2] : LEVEL_AT[2] + 128, :] = jnp.zeros((128, 128), F32)
    add_rows(y)
    place = lax.broadcasted_iota(jnp.int32, (512, 512), 0)
    spot = lax.broadcasted_iota(jnp.int32, (512, 512), 1)
    inner = place % 16
    goal = jnp.where(
        inner < 12,
        place // 16 * 12 + inner,
        jnp.where(inner < 15, 384 + place // 16 * 3 + inner - 12, -1),
    )
    to_map = (goal == spot).astype(BF)

    for came, leg in ((0, 4), (2, 5)):
        y_copy(1, smalls, came).wait_recv()
        y_copy(1, smalls, leg).start()
    for leg in (1, 3):
        y_copy(0, parts, leg).start()
    for came, leg in ((0, 4), (2, 5)):
        y_copy(0, parts, came).wait_recv()
        y_copy(0, parts, leg).start()
    for came in (1, 3, 4, 5):
        y_copy(1, smalls, came).wait_recv()
    coarse[...] = dot(smalls[...].reshape(512, 256), to_map, 0, 0).reshape(HEADS, 32, 512)

    def near_head(h, carry):
        for half in range(2):
            at = slice(half * 128, half * 128 + 128)
            sums = [jnp.zeros((8, 128), F32) for _ in range(4)]
            for point in range(8):
                stride = STRIDE[2 + point // 4]
                anchor = near_i[h, point : point + 1, at]
                for c, off in enumerate((0, 1, stride, stride + 1)):
                    spot = jnp.broadcast_to(anchor + off, (8, 128))
                    lane = spot & 127
                    group = spot >> 7
                    w = jnp.broadcast_to(near_w[h, point * 4 + c : point * 4 + c + 1, at], (8, 128))
                    for v in range(4):

                        def take(g):
                            window = coarse[h, v * 8 : v * 8 + 8, g * 128 : g * 128 + 128]
                            return jnp.take_along_axis(
                                window, lane, axis=1, mode="promise_in_bounds"
                            )

                        if point >= 4:
                            got = take(3)
                        else:
                            got = jnp.where(
                                group == 0, take(0), jnp.where(group == 1, take(1), take(2))
                            )
                        sums[v] = sums[v] + got * w
            near_sum[h, :, at] = jnp.concatenate(sums, axis=0)
        return carry

    lax.fori_loop(0, 4, near_head, 0)
    for came in (1, 3):
        y_copy(0, parts, came).wait_recv()
    add_rows(lax.rem(y + 1, NY))
    add_rows(lax.rem(y + 3, NY))
    for came in (4, 5):
        y_copy(0, parts, came).wait_recv()
    add_rows(lax.rem(y + 2, NY))

    for at, count, stride in zip(LEVEL_AT[:2], LEVEL_ROWS[:2], STRIDE[:2]):
        lane = lax.broadcasted_iota(jnp.int32, (128, 128), 1)

        def four(i, carry, at=at, stride=stride, lane=lane):
            k = pl.multiple_of(at + i * 128, 8)
            c0 = rows[pl.ds(k, 128), :]
            c1 = rows[pl.ds(k + 1, 128), :]
            c2 = rows[pl.ds(pl.multiple_of(k + stride, 8), 128), :]
            c3 = rows[pl.ds(k + stride + 1, 128), :]
            table[pl.ds(k, 128), :] = jnp.where(
                lane < 64, jnp.where(lane < 32, c0, c1), jnp.where(lane < 96, c2, c3)
            )
            return carry

        lax.fori_loop(0, count // 128, four, 0)

    def close(d, bufs):
        done[owner(d)] = (dot(rep, bufs[1][...], 1, 1) + dot(rep, bufs[2][...], 1, 1)).astype(BF)

    def send_back(d):
        @pl.when(d == 0)
        def _():
            heads[z] = done[z]

        @pl.when(d > 0)
        def _():
            h_copy(d).start()

    def stage(d, bufs, other):
        spread, major, minor, ids, _ = bufs

        @pl.when(d < NZ - 1)
        def _():
            i_copy(d + 1).wait_recv()
            fetch(d + 1, other).start()
            w_copy(d + 1).wait_recv()

        fetch(d, bufs).wait()
        other[0][...] = dot(weight[owner(d + 1)], widen, 0, 0)
        for chunk in range(8):
            total = []
            for q0 in range(chunk * 32, chunk * 32 + 32, 8):
                acc = None
                for r in range(8):
                    got = None
                    for k in range(8):
                        one = jnp.broadcast_to(table[pl.ds(ids[r, q0 + k], 1), :], (8, 128))
                        got = one if got is None else jnp.where(sub == k, one, got)
                    term = got * spread[q0 : q0 + 8, r * 128 : r * 128 + 128]
                    acc = term if acc is None else acc + term
                total.append(acc)
            total = jnp.concatenate(total, axis=0)
            top = total.astype(BF)
            major[chunk * 32 : chunk * 32 + 32, :] = top
            minor[chunk * 32 : chunk * 32 + 32, :] = (total - top.astype(F32)).astype(BF)
        close(d - 1, other)

    def pair(i, carry):
        d = 2 * i
        stage(d, set_a, set_b)

        @pl.when(i > 0)
        def _():
            send_back(d - 1)

        stage(d + 1, set_b, set_a)
        send_back(d)
        return carry

    lax.fori_loop(0, NZ // 2, pair, 0)
    close(NZ - 1, set_b)
    send_back(NZ - 1)

    lax.fori_loop(4, HEADS, near_head, 0)
    for c in loads[6:]:
        c.wait()
    for d in range(1, NZ):
        h_copy(d).wait_recv()
    sampled = (
        heads[...].reshape(256, PAD).astype(F32) + near_sum[...].reshape(256, PAD)
    ).astype(BF)
    attended = dot(sampled, w_out[...], 0, 0)[0:BAND_ROWS] + b_out[...]
    middle = layer_norm(feat[...].astype(F32) + attended, gain1[...], shift1[...]).astype(BF)
    hidden = jnp.maximum(dot(middle, w_in[...], 1, 0) + b_in[...], 0.0).astype(BF)
    result = middle.astype(F32) + dot(hidden, w_ff[...], 1, 0) + b_ff[...]
    out[...] = layer_norm(result, gain2[...], shift2[...]).astype(BF)
    for d in range(1, NZ):
        for c in (v_copy(d), i_copy(d), w_copy(d), h_copy(d), s_copy(d)):
            c.wait_send()
    for leg in range(6):
        y_copy(0, parts, leg).wait_send()
        y_copy(1, smalls, leg).wait_send()


def body(
    features, corners, bilinear, attention, w_value, b_value, w_out, b_out,
    norm1_gain, norm1_bias, w_in, b_in, w_ffout, b_ffout, norm2_gain, norm2_bias,
):
    def row(x):
        return x.reshape(1, -1)

    def like(x):
        return VM(x.shape, x.dtype)

    def flat(n):
        return VM((1, n), F32)

    dma = pltpu.SemaphoreType.DMA
    vec = pl.BlockSpec(memory_space=VM)
    return pl.pallas_call(
        layer_kernel,
        out_shape=jax.ShapeDtypeStruct((BAND_ROWS, 256), BF),
        in_specs=[pl.BlockSpec(memory_space=pl.ANY)] * 16,
        out_specs=vec,
        scratch_shapes=[
            like(features), like(corners), like(bilinear), like(attention), like(w_value), flat(256),
            like(w_out), flat(256), flat(256), flat(256), like(w_in), flat(1024), like(w_ffout),
            flat(256), flat(256), flat(256),
            VM((2, 512, 128), jnp.int32),
            VM((HEADS, 32, PAD), BF),
            VM((16, 256), BF),
            VM((HEADS, 8, PAD), jnp.int32),
            VM((HEADS, 32, PAD), BF),
            VM((BANDS, 32, PAD), BF),
            VM((BANDS, 16, 256), BF),
            VM((HEADS, 8, PAD), jnp.int32),
            VM((HEADS, 32, PAD), BF),
            VM((HEADS, 8, PAD), jnp.int32),
            VM((HEADS, 32, PAD), F32),
            VM((HEADS, 32, PAD), F32),
            VM((HEADS, 32, 512), F32),
            VM((LEVEL_AT[2] + 128, 128), F32),
            VM((LEVEL_AT[2], 128), F32),
            VM((PAD, 8 * 128), F32),
            VM((PAD, 8 * 128), F32),
            VM((PAD, 128), BF),
            VM((PAD, 128), BF),
            VM((PAD, 128), BF),
            VM((PAD, 128), BF),
            VM((HEADS, 32, PAD), BF),
            VM((HEADS, 32, PAD), BF),
            pltpu.SMEM((8, PAD), jnp.int32),
            pltpu.SMEM((8, PAD), jnp.int32),
            dma((16,)),
            dma((2,)),
            dma((5, NZ)),
            dma((5, NZ)),
            dma((2, 6)),
            dma((2, 6)),
        ],
        compiler_params=pltpu.CompilerParams(
            collective_id=0, has_side_effects=True, vmem_limit_bytes=60 << 20
        ),
        name="layer",
    )(
        features, corners, bilinear, attention, w_value, row(b_value), w_out, row(b_out),
        row(norm1_gain), row(norm1_bias), w_in, row(b_in), w_ffout, row(b_ffout),
        row(norm2_gain), row(norm2_bias),
    )


def solution(mesh):
    split = Mesh(mesh.devices.reshape(mesh.shape["dp"], NY, NZ), DP_BAND)
    return jax.shard_map(
        body,
        mesh=split,
        in_specs=(P(DP_BAND, None),) * 4 + (P(),) * 12,
        out_specs=P(DP_BAND, None),
        check_vma=False,
    )
```

```python
import jax
import jax.numpy as jnp
from jax import lax
from jax.experimental import pallas as pl
from jax.experimental.pallas import tpu as pltpu
from jax.sharding import Mesh
from jax.sharding import PartitionSpec as P

MESH_ID = pl.DeviceIdType.MESH
DP_BAND = ("dp", "band_0", "band_1")
HEADS = 8
NY, NZ = 4, 8
BANDS = NY * NZ
BAND_ROWS = 255
PAD = 256
LEVEL_ROWS = (6144, 1536, 384, 96)
LEVEL_AT = (0, 6144, 7680, 8064)
STRIDE = (128, 64, 32, 16)
BAND_PART = (192, 48, 12, 3)
BAND_AT = (0, 192, 240, 252)
TOKENS = 8160
POINTS = 16
FAR_FIRST = (4, 3, 5, 2, 6, 1, 7)
BF = jnp.bfloat16
F32 = jnp.float32
VM = pltpu.VMEM


def dot(a, b, ca, cb, precision=None):
    return lax.dot_general(
        a, b, (((ca,), (cb,)), ((), ())), preferred_element_type=F32, precision=precision
    )


def onehot(rows, columns, hit):
    r = lax.broadcasted_iota(jnp.int32, (rows, columns), 0)
    c = lax.broadcasted_iota(jnp.int32, (rows, columns), 1)
    return hit(r, c).astype(BF)


def layer_norm(inputs, gain, shift):
    average = jnp.mean(inputs, axis=-1, keepdims=True)
    centred = inputs - average
    variance = jnp.mean(centred * centred, axis=-1, keepdims=True)
    return centred * lax.rsqrt(variance + 1e-05) * gain + shift


def layer_kernel(
    feat_in, corner_in, bil_in, att_in, w_value_in, b_value_in, w_out_in, b_out_in, gain1_in, shift1_in,
    w_in_in, b_in_in, w_ff_in, b_ff_in, gain2_in, shift2_in,
    out,
    feat, corner, bil, att, w_value, b_value, w_out, b_out, gain1, shift1, w_in, b_in, w_ff, b_ff,
    gain2, shift2, turned_ids,
    send_v, send_s, send_i, send_w, parts, smalls, index, weight, near_i, near_w, near_sum, coarse,
    rows, table, spread_a, spread_b, major_a, major_b, minor_a, minor_b, done, heads, ids_a, ids_b,
    load_sem, ids_sem, sems_out, sems_in, y_out, y_in,
):
    y = lax.axis_index("band_0")
    z = lax.axis_index("band_1")
    here = y * NZ + z
    barrier = pltpu.get_barrier_semaphore()
    for d in range(1, NZ):
        pl.semaphore_signal(
            barrier, inc=1, device_id={"band_1": lax.rem(z + d, NZ)}, device_id_type=MESH_ID
        )
    for d in (1, NY - 1):
        pl.semaphore_signal(
            barrier, inc=1, device_id={"band_0": lax.rem(y + d, NY)}, device_id_type=MESH_ID
        )
    loads = [
        pltpu.make_async_copy(src, dst, load_sem.at[i])
        for i, (src, dst) in enumerate(
            (
                (feat_in, feat), (w_value_in, w_value), (b_value_in, b_value), (corner_in, corner),
                (att_in, att), (bil_in, bil), (w_out_in, w_out), (b_out_in, b_out),
                (gain1_in, gain1), (shift1_in, shift1), (w_in_in, w_in), (b_in_in, b_in),
                (w_ff_in, w_ff), (b_ff_in, b_ff), (gain2_in, gain2), (shift2_in, shift2),
            )
        )
    ]
    for c in loads[0:3]:
        c.start()

    def z_copy(kind, src, dst, slot, d, back=False):
        t = lax.rem(z + NZ - d, NZ) if back else lax.rem(z + d, NZ)
        return pltpu.make_async_remote_copy(
            src_ref=src if src is send_s else src.at[t],
            dst_ref=dst.at[slot],
            send_sem=sems_out.at[kind, d],
            recv_sem=sems_in.at[kind, d],
            device_id={"band_1": t},
            device_id_type=MESH_ID,
        )

    def v_copy(d):
        return z_copy(0, send_v, parts, here, d)

    def i_copy(d):
        return z_copy(1, send_i, index, z, d)

    def w_copy(d):
        return z_copy(2, send_w, weight, z, d)

    def h_copy(d):
        return z_copy(3, done, heads, z, d, back=True)

    def s_copy(d):
        return z_copy(4, send_s, smalls, here, d)

    def y_copy(kind, ref, leg):
        step = (1, 1, NY - 1, NY - 1, 1, NY - 1)[leg]
        column = (y, y, y, y, lax.rem(y + NY - 1, NY), lax.rem(y + 1, NY))[leg]
        half = (0, 1, 1, 0, 0, 1)[leg]
        piece = ref.at[pl.ds(column * NZ + half * (NZ // 2), NZ // 2)]
        return pltpu.make_async_remote_copy(
            src_ref=piece,
            dst_ref=piece,
            send_sem=y_out.at[kind, leg],
            recv_sem=y_in.at[kind, leg],
            device_id={"band_0": lax.rem(y + step, NY)},
            device_id_type=MESH_ID,
        )

    for c in loads[0:3]:
        c.wait()
    for c in loads[3:]:
        c.start()
    values = (dot(feat[...], w_value[...], 1, 0) + b_value[...]).astype(BF)
    eye = onehot(256, 256, lambda r, c: r == c)
    turned = dot(eye, values, 1, 1).astype(BF)
    send_s[...] = jnp.zeros((16, 256), BF)
    send_s[0:15, :] = values[BAND_AT[2] : BAND_ROWS, :]
    send_v[:, :, 0:BAND_ROWS] = turned.reshape(HEADS, 32, BAND_ROWS)
    pl.semaphore_wait(barrier, NZ + 1)
    for d in FAR_FIRST:
        s_copy(d).start()
    for d in FAR_FIRST:
        v_copy(d).start()
    parts[here] = send_v[z]
    smalls[here] = send_s[...]

    loads[3].wait()
    turned_ids[0, :, :] = jnp.transpose(corner[0:128, :])
    turned_ids[1, :, 0 : BAND_ROWS - 128] = jnp.transpose(corner[128:BAND_ROWS, :])
    level = (lax.broadcasted_iota(jnp.int32, (128, 128), 0) // 4) % 4
    base = jnp.where(
        level == 0, LEVEL_AT[0], jnp.where(level == 1, LEVEL_AT[1], jnp.where(level == 2, 0, 384))
    )
    used = lax.broadcasted_iota(jnp.int32, (128, 128), 1) < BAND_ROWS - 128
    left = turned_ids[0, pl.ds(0, 128, stride=4), :] + base
    right = jnp.where(used, turned_ids[1, pl.ds(0, 128, stride=4), :] + base, 0)
    for at, side in ((0, left), (128, right)):
        side = side.reshape(HEADS, POINTS, 128)
        send_i[:, :, at : at + 128] = side[:, 0:8]
        near_i[:, :, at : at + 128] = side[:, 8:16]
    for d in FAR_FIRST:
        i_copy(d).start()
    index[z] = send_i[z]

    loads[4].wait()
    loads[5].wait()
    repeat = onehot(128, 512, lambda r, c: c // 4 == r)
    whole = att[...]
    first = whole.astype(BF)
    rest = whole - first.astype(F32)
    second = rest.astype(BF)
    third = (rest - second.astype(F32)).astype(BF)
    each = dot(first, repeat, 1, 0) + dot(second, repeat, 1, 0) + dot(third, repeat, 1, 0)
    product = (each * bil[...]).astype(BF)
    eye2 = onehot(512, 512, lambda r, c: r == c)
    turned_w = dot(eye2, product, 1, 1).reshape(HEADS, 64, BAND_ROWS)
    send_w[:, :, 0:BAND_ROWS] = turned_w[:, 0:32].astype(BF)
    near_w[:, :, 0:BAND_ROWS] = turned_w[:, 32:64]
    for d in FAR_FIRST:
        w_copy(d).start()
    weight[z] = send_w[z]

    widen = onehot(32, 8 * 128, lambda r, c: c // 32 == r)
    sub = lax.broadcasted_iota(jnp.int32, (8, 128), 0)
    set_a = (spread_a, major_a, minor_a, ids_a, 0)
    set_b = (spread_b, major_b, minor_b, ids_b, 1)

    def owner(d):
        return lax.rem(z + 2 * NZ - d, NZ)

    def fetch(d, bufs):
        return pltpu.make_async_copy(index.at[owner(d)], bufs[3], ids_sem.at[bufs[4]])

    spread_a[...] = dot(weight[z], widen, 0, 0)
    major_b[...] = jnp.zeros((PAD, 128), BF)
    minor_b[...] = jnp.zeros((PAD, 128), BF)
    fetch(0, set_a).start()

    for d in range(1, NZ):
        s_copy(d).wait_recv()
    for leg in range(4):
        y_copy(1, smalls, leg).start()
    rep = onehot(32, 128, lambda r, c: c % 32 == r)
    for d in range(1, NZ):
        v_copy(d).wait_recv()
    for leg in (0, 2):
        y_copy(0, parts, leg).start()

    def add_rows(column):
        for i in range(NZ):
            b = column * NZ + i
            wide = dot(parts[b], rep, 0, 0)
            for at, count, begin in zip(LEVEL_AT[:2], BAND_PART[:2], BAND_AT[:2]):
                rows[pl.ds(pl.multiple_of(at + b * count, 16), count), :] = wide[
                    begin : begin + count, :
                ]

    rows[LEVEL_AT[2] : LEVEL_AT[2] + 128, :] = jnp.zeros((128, 128), F32)
    add_rows(y)
    place = lax.broadcasted_iota(jnp.int32, (512, 512), 0)
    spot = lax.broadcasted_iota(jnp.int32, (512, 512), 1)
    inner = place % 16
    goal = jnp.where(
        inner < 12,
        place // 16 * 12 + inner,
        jnp.where(inner < 15, 384 + place // 16 * 3 + inner - 12, -1),
    )
    to_map = (goal == spot).astype(BF)

    for came, leg in ((0, 4), (2, 5)):
        y_copy(1, smalls, came).wait_recv()
        y_copy(1, smalls, leg).start()
    for leg in (1, 3):
        y_copy(0, parts, leg).start()
    for came, leg in ((0, 4), (2, 5)):
        y_copy(0, parts, came).wait_recv()
        y_copy(0, parts, leg).start()
    for came in (1, 3, 4, 5):
        y_copy(1, smalls, came).wait_recv()
    coarse[...] = dot(smalls[...].reshape(512, 256), to_map, 0, 0).reshape(HEADS, 32, 512)

    def near_head(h, carry):
        for half in range(2):
            at = slice(half * 128, half * 128 + 128)
            sums = [jnp.zeros((8, 128), F32) for _ in range(4)]
            for point in range(8):
                stride = STRIDE[2 + point // 4]
                anchor = near_i[h, point : point + 1, at]
                for c, off in enumerate((0, 1, stride, stride + 1)):
                    spot = jnp.broadcast_to(anchor + off, (8, 128))
                    lane = spot & 127
                    group = spot >> 7
                    w = jnp.broadcast_to(near_w[h, point * 4 + c : point * 4 + c + 1, at], (8, 128))
                    for v in range(4):

                        def take(g):
                            window = coarse[h, v * 8 : v * 8 + 8, g * 128 : g * 128 + 128]
                            return jnp.take_along_axis(
                                window, lane, axis=1, mode="promise_in_bounds"
                            )

                        if point >= 4:
                            got = take(3)
                        else:
                            got = jnp.where(
                                group == 0, take(0), jnp.where(group == 1, take(1), take(2))
                            )
                        sums[v] = sums[v] + got * w
            near_sum[h, :, at] = jnp.concatenate(sums, axis=0)
        return carry

    lax.fori_loop(0, 3, near_head, 0)
    for came in (1, 3):
        y_copy(0, parts, came).wait_recv()
    add_rows(lax.rem(y + 1, NY))
    add_rows(lax.rem(y + 3, NY))
    for came in (4, 5):
        y_copy(0, parts, came).wait_recv()
    add_rows(lax.rem(y + 2, NY))

    for at, count, stride in zip(LEVEL_AT[:2], LEVEL_ROWS[:2], STRIDE[:2]):
        lane = lax.broadcasted_iota(jnp.int32, (128, 128), 1)

        def four(i, carry, at=at, stride=stride, lane=lane):
            k = pl.multiple_of(at + i * 128, 8)
            c0 = rows[pl.ds(k, 128), :]
            c1 = rows[pl.ds(k + 1, 128), :]
            c2 = rows[pl.ds(pl.multiple_of(k + stride, 8), 128), :]
            c3 = rows[pl.ds(k + stride + 1, 128), :]
            table[pl.ds(k, 128), :] = jnp.where(
                lane < 64, jnp.where(lane < 32, c0, c1), jnp.where(lane < 96, c2, c3)
            )
            return carry

        lax.fori_loop(0, count // 128, four, 0)

    def close(d, bufs):
        done[owner(d)] = (dot(rep, bufs[1][...], 1, 1) + dot(rep, bufs[2][...], 1, 1)).astype(BF)

    def send_back(d):
        @pl.when(d == 0)
        def _():
            heads[z] = done[z]

        @pl.when(d > 0)
        def _():
            h_copy(d).start()

    def stage(d, bufs, other):
        spread, major, minor, ids, _ = bufs

        @pl.when(d < NZ - 1)
        def _():
            i_copy(d + 1).wait_recv()
            fetch(d + 1, other).start()
            w_copy(d + 1).wait_recv()

        fetch(d, bufs).wait()
        other[0][...] = dot(weight[owner(d + 1)], widen, 0, 0)
        for chunk in range(8):
            total = []
            for q0 in range(chunk * 32, chunk * 32 + 32, 8):
                acc = None
                for r in range(8):
                    got = None
                    for k in range(8):
                        one = jnp.broadcast_to(table[pl.ds(ids[r, q0 + k], 1), :], (8, 128))
                        got = one if got is None else jnp.where(sub == k, one, got)
                    term = got * spread[q0 : q0 + 8, r * 128 : r * 128 + 128]
                    acc = term if acc is None else acc + term
                total.append(acc)
            total = jnp.concatenate(total, axis=0)
            top = total.astype(BF)
            major[chunk * 32 : chunk * 32 + 32, :] = top
            minor[chunk * 32 : chunk * 32 + 32, :] = (total - top.astype(F32)).astype(BF)
        close(d - 1, other)

    def pair(i, carry):
        d = 2 * i
        stage(d, set_a, set_b)

        @pl.when(i > 0)
        def _():
            send_back(d - 1)

        stage(d + 1, set_b, set_a)
        send_back(d)
        return carry

    lax.fori_loop(0, NZ // 2, pair, 0)
    close(NZ - 1, set_b)
    send_back(NZ - 1)

    lax.fori_loop(3, HEADS, near_head, 0)
    for c in loads[6:]:
        c.wait()
    for d in range(1, NZ):
        h_copy(d).wait_recv()
    sampled = (
        heads[...].reshape(256, PAD).astype(F32) + near_sum[...].reshape(256, PAD)
    ).astype(BF)
    attended = dot(sampled, w_out[...], 0, 0)[0:BAND_ROWS] + b_out[...]
    middle = layer_norm(feat[...].astype(F32) + attended, gain1[...], shift1[...]).astype(BF)
    hidden = jnp.maximum(dot(middle, w_in[...], 1, 0) + b_in[...], 0.0).astype(BF)
    result = middle.astype(F32) + dot(hidden, w_ff[...], 1, 0) + b_ff[...]
    out[...] = layer_norm(result, gain2[...], shift2[...]).astype(BF)
    for d in range(1, NZ):
        for c in (v_copy(d), i_copy(d), w_copy(d), h_copy(d), s_copy(d)):
            c.wait_send()
    for leg in range(6):
        y_copy(0, parts, leg).wait_send()
        y_copy(1, smalls, leg).wait_send()


def body(
    features, corners, bilinear, attention, w_value, b_value, w_out, b_out,
    norm1_gain, norm1_bias, w_in, b_in, w_ffout, b_ffout, norm2_gain, norm2_bias,
):
    def row(x):
        return x.reshape(1, -1)

    def like(x):
        return VM(x.shape, x.dtype)

    def flat(n):
        return VM((1, n), F32)

    dma = pltpu.SemaphoreType.DMA
    vec = pl.BlockSpec(memory_space=VM)
    return pl.pallas_call(
        layer_kernel,
        out_shape=jax.ShapeDtypeStruct((BAND_ROWS, 256), BF),
        in_specs=[pl.BlockSpec(memory_space=pl.ANY)] * 16,
        out_specs=vec,
        scratch_shapes=[
            like(features), like(corners), like(bilinear), like(attention), like(w_value), flat(256),
            like(w_out), flat(256), flat(256), flat(256), like(w_in), flat(1024), like(w_ffout),
            flat(256), flat(256), flat(256),
            VM((2, 512, 128), jnp.int32),
            VM((HEADS, 32, PAD), BF),
            VM((16, 256), BF),
            VM((HEADS, 8, PAD), jnp.int32),
            VM((HEADS, 32, PAD), BF),
            VM((BANDS, 32, PAD), BF),
            VM((BANDS, 16, 256), BF),
            VM((HEADS, 8, PAD), jnp.int32),
            VM((HEADS, 32, PAD), BF),
            VM((HEADS, 8, PAD), jnp.int32),
            VM((HEADS, 32, PAD), F32),
            VM((HEADS, 32, PAD), F32),
            VM((HEADS, 32, 512), F32),
            VM((LEVEL_AT[2] + 128, 128), F32),
            VM((LEVEL_AT[2], 128), F32),
            VM((PAD, 8 * 128), F32),
            VM((PAD, 8 * 128), F32),
            VM((PAD, 128), BF),
            VM((PAD, 128), BF),
            VM((PAD, 128), BF),
            VM((PAD, 128), BF),
            VM((HEADS, 32, PAD), BF),
            VM((HEADS, 32, PAD), BF),
            pltpu.SMEM((8, PAD), jnp.int32),
            pltpu.SMEM((8, PAD), jnp.int32),
            dma((16,)),
            dma((2,)),
            dma((5, NZ)),
            dma((5, NZ)),
            dma((2, 6)),
            dma((2, 6)),
        ],
        compiler_params=pltpu.CompilerParams(
            collective_id=0, has_side_effects=True, vmem_limit_bytes=60 << 20
        ),
        name="layer",
    )(
        features, corners, bilinear, attention, w_value, row(b_value), w_out, row(b_out),
        row(norm1_gain), row(norm1_bias), w_in, row(b_in), w_ffout, row(b_ffout),
        row(norm2_gain), row(norm2_bias),
    )


def solution(mesh):
    split = Mesh(mesh.devices.reshape(mesh.shape["dp"], NY, NZ), DP_BAND)
    return jax.shard_map(
        body,
        mesh=split,
        in_specs=(P(DP_BAND, None),) * 4 + (P(),) * 12,
        out_specs=P(DP_BAND, None),
        check_vma=False,
    )
```

```python
import jax
import jax.numpy as jnp
from jax import lax
from jax.experimental import pallas as pl
from jax.experimental.pallas import tpu as pltpu
from jax.sharding import Mesh
from jax.sharding import PartitionSpec as P

MESH_ID = pl.DeviceIdType.MESH
DP_BAND = ("dp", "band_0", "band_1")
HEADS = 8
NY, NZ = 4, 8
BANDS = NY * NZ
BAND_ROWS = 255
PAD = 256
LEVEL_ROWS = (6144, 1536, 384, 96)
LEVEL_AT = (0, 6144, 7680, 8064)
STRIDE = (128, 64, 32, 16)
BAND_PART = (192, 48, 12, 3)
BAND_AT = (0, 192, 240, 252)
TOKENS = 8160
POINTS = 16
FAR_FIRST = (4, 3, 5, 2, 6, 1, 7)
BF = jnp.bfloat16
F32 = jnp.float32
VM = pltpu.VMEM


def dot(a, b, ca, cb, precision=None):
    return lax.dot_general(
        a, b, (((ca,), (cb,)), ((), ())), preferred_element_type=F32, precision=precision
    )


def onehot(rows, columns, hit):
    r = lax.broadcasted_iota(jnp.int32, (rows, columns), 0)
    c = lax.broadcasted_iota(jnp.int32, (rows, columns), 1)
    return hit(r, c).astype(BF)


def layer_norm(inputs, gain, shift):
    average = jnp.mean(inputs, axis=-1, keepdims=True)
    centred = inputs - average
    variance = jnp.mean(centred * centred, axis=-1, keepdims=True)
    return centred * lax.rsqrt(variance + 1e-05) * gain + shift


def lanes_of(window, lane):
    return lax.gather(
        window,
        lane[..., None],
        lax.GatherDimensionNumbers(
            offset_dims=(),
            collapsed_slice_dims=(1,),
            start_index_map=(1,),
            operand_batching_dims=(0,),
            start_indices_batching_dims=(0,),
        ),
        slice_sizes=(1, 1),
        mode=lax.GatherScatterMode.PROMISE_IN_BOUNDS,
    )


def layer_kernel(
    feat_in, corner_in, bil_in, att_in, w_value_in, b_value_in, w_out_in, b_out_in, gain1_in, shift1_in,
    w_in_in, b_in_in, w_ff_in, b_ff_in, gain2_in, shift2_in,
    out,
    feat, corner, bil, att, w_value, b_value, w_out, b_out, gain1, shift1, w_in, b_in, w_ff, b_ff,
    gain2, shift2, turned_ids,
    send_v, send_s, send_i, send_w, parts, smalls, index, weight, near_i, near_w, near_sum, coarse,
    rows, table, spread_a, spread_b, major_a, major_b, minor_a, minor_b, done, heads, ids_a, ids_b,
    load_sem, ids_sem, sems_out, sems_in, y_out, y_in,
):
    y = lax.axis_index("band_0")
    z = lax.axis_index("band_1")
    here = y * NZ + z
    barrier = pltpu.get_barrier_semaphore()
    for d in range(1, NZ):
        pl.semaphore_signal(
            barrier, inc=1, device_id={"band_1": lax.rem(z + d, NZ)}, device_id_type=MESH_ID
        )
    for d in (1, NY - 1):
        pl.semaphore_signal(
            barrier, inc=1, device_id={"band_0": lax.rem(y + d, NY)}, device_id_type=MESH_ID
        )
    loads = [
        pltpu.make_async_copy(src, dst, load_sem.at[i])
        for i, (src, dst) in enumerate(
            (
                (feat_in, feat), (w_value_in, w_value), (b_value_in, b_value), (corner_in, corner),
                (att_in, att), (bil_in, bil), (w_out_in, w_out), (b_out_in, b_out),
                (gain1_in, gain1), (shift1_in, shift1), (w_in_in, w_in), (b_in_in, b_in),
                (w_ff_in, w_ff), (b_ff_in, b_ff), (gain2_in, gain2), (shift2_in, shift2),
            )
        )
    ]
    for c in loads[0:3]:
        c.start()

    def z_copy(kind, src, dst, slot, d, back=False):
        t = lax.rem(z + NZ - d, NZ) if back else lax.rem(z + d, NZ)
        return pltpu.make_async_remote_copy(
            src_ref=src if src is send_s else src.at[t],
            dst_ref=dst.at[slot],
            send_sem=sems_out.at[kind, d],
            recv_sem=sems_in.at[kind, d],
            device_id={"band_1": t},
            device_id_type=MESH_ID,
        )

    def v_copy(d):
        return z_copy(0, send_v, parts, here, d)

    def i_copy(d):
        return z_copy(1, send_i, index, z, d)

    def w_copy(d):
        return z_copy(2, send_w, weight, z, d)

    def h_copy(d):
        return z_copy(3, done, heads, z, d, back=True)

    def s_copy(d):
        return z_copy(4, send_s, smalls, here, d)

    above, below = lax.rem(y + 1, NY), lax.rem(y + NY - 1, NY)
    legs = (
        (
            (1, y, 0, 4), (1, y, 4, 4), (NY - 1, y, 4, 4), (NY - 1, y, 0, 4),
            (1, below, 0, 4), (NY - 1, above, 4, 4),
        ),
        (
            (1, y, 0, 2), (1, y, 2, 2), (NY - 1, y, 4, 2), (NY - 1, y, 6, 2),
            (1, y, 4, 4), (NY - 1, y, 0, 4),
            (1, below, 0, 2), (NY - 1, above, 4, 2), (1, below, 2, 2), (NY - 1, above, 6, 2),
        ),
    )

    def y_copy(kind, leg):
        step, column, begin, count = legs[kind][leg]
        piece = (smalls, parts)[kind].at[pl.ds(column * NZ + begin, count)]
        return pltpu.make_async_remote_copy(
            src_ref=piece,
            dst_ref=piece,
            send_sem=y_out.at[kind, leg],
            recv_sem=y_in.at[kind, leg],
            device_id={"band_0": lax.rem(y + step, NY)},
            device_id_type=MESH_ID,
        )

    for c in loads[0:3]:
        c.wait()
    for c in loads[3:]:
        c.start()
    values = (dot(feat[...], w_value[...], 1, 0) + b_value[...]).astype(BF)
    eye = onehot(256, 256, lambda r, c: r == c)
    turned = dot(eye, values, 1, 1).astype(BF)
    send_s[...] = jnp.zeros((16, 256), BF)
    send_s[0:15, :] = values[BAND_AT[2] : BAND_ROWS, :]
    send_v[:, :, 0:BAND_ROWS] = turned.reshape(HEADS, 32, BAND_ROWS)
    pl.semaphore_wait(barrier, NZ + 1)
    for d in FAR_FIRST:
        s_copy(d).start()
    for d in FAR_FIRST:
        v_copy(d).start()
    parts[here] = send_v[z]
    smalls[here] = send_s[...]

    loads[3].wait()
    turned_ids[0, :, :] = jnp.transpose(corner[0:128, :])
    turned_ids[1, :, 0 : BAND_ROWS - 128] = jnp.transpose(corner[128:BAND_ROWS, :])
    level = (lax.broadcasted_iota(jnp.int32, (128, 128), 0) // 4) % 4
    base = jnp.where(
        level == 0, LEVEL_AT[0], jnp.where(level == 1, LEVEL_AT[1], jnp.where(level == 2, 0, 384))
    )
    used = lax.broadcasted_iota(jnp.int32, (128, 128), 1) < BAND_ROWS - 128
    left = turned_ids[0, pl.ds(0, 128, stride=4), :] + base
    right = jnp.where(used, turned_ids[1, pl.ds(0, 128, stride=4), :] + base, 0)
    for at, side in ((0, left), (128, right)):
        side = side.reshape(HEADS, POINTS, 128)
        send_i[:, :, at : at + 128] = side[:, 0:8]
        near_i[:, :, at : at + 128] = side[:, 8:16]
    for d in FAR_FIRST:
        i_copy(d).start()
    index[z] = send_i[z]

    loads[4].wait()
    loads[5].wait()
    repeat = onehot(128, 512, lambda r, c: c // 4 == r)
    whole = att[...]
    first = whole.astype(BF)
    rest = whole - first.astype(F32)
    second = rest.astype(BF)
    third = (rest - second.astype(F32)).astype(BF)
    each = dot(first, repeat, 1, 0) + dot(second, repeat, 1, 0) + dot(third, repeat, 1, 0)
    product = (each * bil[...]).astype(BF)
    eye2 = onehot(512, 512, lambda r, c: r == c)
    turned_w = dot(eye2, product, 1, 1).reshape(HEADS, 64, BAND_ROWS)
    send_w[:, :, 0:BAND_ROWS] = turned_w[:, 0:32].astype(BF)
    near_w[:, :, 0:BAND_ROWS] = turned_w[:, 32:64]
    for d in FAR_FIRST:
        w_copy(d).start()
    weight[z] = send_w[z]

    widen = onehot(32, 8 * 128, lambda r, c: c // 32 == r)
    sub = lax.broadcasted_iota(jnp.int32, (8, 128), 0)
    set_a = (spread_a, major_a, minor_a, ids_a, 0)
    set_b = (spread_b, major_b, minor_b, ids_b, 1)

    def owner(d):
        return lax.rem(z + 2 * NZ - 1 - d, NZ)

    def fetch(d, bufs):
        return pltpu.make_async_copy(index.at[owner(d)], bufs[3], ids_sem.at[bufs[4]])

    major_b[...] = jnp.zeros((PAD, 128), BF)
    minor_b[...] = jnp.zeros((PAD, 128), BF)

    for d in range(1, NZ):
        s_copy(d).wait_recv()
    for leg in range(4):
        y_copy(0, leg).start()
    rep = onehot(32, 128, lambda r, c: c % 32 == r)
    for d in range(1, NZ):
        v_copy(d).wait_recv()
    for leg in (0, 2, 1, 3):
        y_copy(1, leg).start()

    def add_rows(column):
        for i in range(NZ):
            b = column * NZ + i
            wide = dot(parts[b], rep, 0, 0)
            for at, count, begin in zip(LEVEL_AT[:2], BAND_PART[:2], BAND_AT[:2]):
                rows[pl.ds(pl.multiple_of(at + b * count, 16), count), :] = wide[
                    begin : begin + count, :
                ]

    def four(start, count, level):
        stride = STRIDE[level]
        lane = lax.broadcasted_iota(jnp.int32, (128, 128), 1)

        def chunk(i, carry):
            k = (start + i) * 128
            k = jnp.where(k >= LEVEL_ROWS[level], k - LEVEL_ROWS[level], k) + LEVEL_AT[level]
            k = pl.multiple_of(k, 128)
            c0 = rows[pl.ds(k, 128), :]
            c1 = rows[pl.ds(k + 1, 128), :]
            c2 = rows[pl.ds(pl.multiple_of(k + stride, 8), 128), :]
            c3 = rows[pl.ds(k + stride + 1, 128), :]
            table[pl.ds(k, 128), :] = jnp.where(
                lane < 64, jnp.where(lane < 32, c0, c1), jnp.where(lane < 96, c2, c3)
            )
            return carry

        lax.fori_loop(0, count, chunk, 0)

    rows[LEVEL_AT[2] : LEVEL_AT[2] + 128, :] = jnp.zeros((128, 128), F32)
    add_rows(y)
    place = lax.broadcasted_iota(jnp.int32, (512, 512), 0)
    spot = lax.broadcasted_iota(jnp.int32, (512, 512), 1)
    inner = place % 16
    goal = jnp.where(
        inner < 12,
        place // 16 * 12 + inner,
        jnp.where(inner < 15, 384 + place // 16 * 3 + inner - 12, -1),
    )
    to_map = (goal == spot).astype(BF)

    for came, leg in ((0, 4), (2, 5)):
        y_copy(0, came).wait_recv()
        y_copy(0, leg).start()
    for leg in (4, 5):
        y_copy(1, leg).start()
    for came, leg in ((0, 6), (2, 7), (1, 8), (3, 9)):
        y_copy(1, came).wait_recv()
        y_copy(1, leg).start()
    i_copy(1).wait_recv()
    fetch(0, set_a).start()
    w_copy(1).wait_recv()
    spread_a[...] = dot(weight[owner(0)], widen, 0, 0)
    for came in (1, 3, 4, 5):
        y_copy(0, came).wait_recv()
    coarse[...] = dot(smalls[...].reshape(512, 256), to_map, 0, 0).astype(BF).reshape(
        HEADS, 32, 512
    )

    def near_head(h, carry):
        for half in range(2):
            at = slice(half * 128, half * 128 + 128)
            sums = [jnp.zeros((16, 128), F32) for _ in range(2)]
            for point in range(8):
                stride = STRIDE[2 + point // 4]
                anchor = jnp.broadcast_to(near_i[h, point : point + 1, at], (16, 128)).astype(
                    jnp.int16
                )
                for c, off in enumerate((0, 1, stride, stride + 1)):
                    spot = anchor + jnp.int16(off)
                    lane = spot & jnp.int16(127)
                    w = jnp.broadcast_to(
                        near_w[h, point * 4 + c : point * 4 + c + 1, at], (16, 128)
                    )
                    for v in range(2):

                        def take(g):
                            return lanes_of(
                                coarse[h, v * 16 : v * 16 + 16, g * 128 : g * 128 + 128], lane
                            )

                        if point >= 4:
                            got = take(3)
                        else:
                            got = jnp.where(
                                spot < 128, take(0), jnp.where(spot < 256, take(1), take(2))
                            )
                        sums[v] = sums[v] + got.astype(F32) * w
            near_sum[h, :, at] = jnp.concatenate(sums, axis=0)
        return carry

    lax.fori_loop(0, 2, near_head, 0)
    for came in (4, 5):
        y_copy(1, came).wait_recv()
    add_rows(lax.rem(y + 1, NY))
    add_rows(lax.rem(y + 3, NY))
    four(lax.rem(y + 3, NY) * 12, 34, 0)
    four(lax.rem(y + 3, NY) * 3, 8, 1)
    for came in (6, 7, 8, 9):
        y_copy(1, came).wait_recv()
    add_rows(lax.rem(y + 2, NY))

    four(lax.rem(y + 1, NY) * 12 + 10, 14, 0)
    four(lax.rem(y + 1, NY) * 3 + 2, 4, 1)

    def close(d, bufs):
        done[owner(d)] = (dot(rep, bufs[1][...], 1, 1) + dot(rep, bufs[2][...], 1, 1)).astype(BF)

    def send_back(d):
        h_copy(d + 1).start()

    def stage(d, bufs, other):
        spread, major, minor, ids, _ = bufs

        @pl.when(d < NZ - 2)
        def _():
            i_copy(d + 2).wait_recv()
            w_copy(d + 2).wait_recv()

        @pl.when(d < NZ - 1)
        def _():
            fetch(d + 1, other).start()

        fetch(d, bufs).wait()
        other[0][...] = dot(weight[owner(d + 1)], widen, 0, 0)
        for chunk in range(8):
            total = []
            for q0 in range(chunk * 32, chunk * 32 + 32, 8):
                acc = None
                for r in range(8):
                    got = None
                    for k in range(8):
                        one = jnp.broadcast_to(table[pl.ds(ids[r, q0 + k], 1), :], (8, 128))
                        got = one if got is None else jnp.where(sub == k, one, got)
                    term = got * spread[q0 : q0 + 8, r * 128 : r * 128 + 128]
                    acc = term if acc is None else acc + term
                total.append(acc)
            total = jnp.concatenate(total, axis=0)
            top = total.astype(BF)
            major[chunk * 32 : chunk * 32 + 32, :] = top
            minor[chunk * 32 : chunk * 32 + 32, :] = (total - top.astype(F32)).astype(BF)
        close(d - 1, other)

    def pair(i, carry):
        d = 2 * i
        stage(d, set_a, set_b)

        @pl.when(i > 0)
        def _():
            send_back(d - 1)

        stage(d + 1, set_b, set_a)
        send_back(d)
        return carry

    lax.fori_loop(0, NZ // 2, pair, 0)
    close(NZ - 1, set_b)
    heads[z] = done[z]

    lax.fori_loop(2, HEADS, near_head, 0)
    for c in loads[6:]:
        c.wait()
    for d in range(1, NZ):
        h_copy(d).wait_recv()
    sampled = (
        heads[...].reshape(256, PAD).astype(F32) + near_sum[...].reshape(256, PAD)
    ).astype(BF)
    attended = dot(sampled, w_out[...], 0, 0)[0:BAND_ROWS] + b_out[...]
    middle = layer_norm(feat[...].astype(F32) + attended, gain1[...], shift1[...]).astype(BF)
    hidden = jnp.maximum(dot(middle, w_in[...], 1, 0) + b_in[...], 0.0).astype(BF)
    result = middle.astype(F32) + dot(hidden, w_ff[...], 1, 0) + b_ff[...]
    out[...] = layer_norm(result, gain2[...], shift2[...]).astype(BF)
    for d in range(1, NZ):
        for c in (v_copy(d), i_copy(d), w_copy(d), h_copy(d), s_copy(d)):
            c.wait_send()
    for kind in range(2):
        for leg in range(len(legs[kind])):
            y_copy(kind, leg).wait_send()


def body(
    features, corners, bilinear, attention, w_value, b_value, w_out, b_out,
    norm1_gain, norm1_bias, w_in, b_in, w_ffout, b_ffout, norm2_gain, norm2_bias,
):
    def row(x):
        return x.reshape(1, -1)

    def like(x):
        return VM(x.shape, x.dtype)

    def flat(n):
        return VM((1, n), F32)

    dma = pltpu.SemaphoreType.DMA
    vec = pl.BlockSpec(memory_space=VM)
    return pl.pallas_call(
        layer_kernel,
        out_shape=jax.ShapeDtypeStruct((BAND_ROWS, 256), BF),
        in_specs=[pl.BlockSpec(memory_space=pl.ANY)] * 16,
        out_specs=vec,
        scratch_shapes=[
            like(features), like(corners), like(bilinear), like(attention), like(w_value), flat(256),
            like(w_out), flat(256), flat(256), flat(256), like(w_in), flat(1024), like(w_ffout),
            flat(256), flat(256), flat(256),
            VM((2, 512, 128), jnp.int32),
            VM((HEADS, 32, PAD), BF),
            VM((16, 256), BF),
            VM((HEADS, 8, PAD), jnp.int32),
            VM((HEADS, 32, PAD), BF),
            VM((BANDS, 32, PAD), BF),
            VM((BANDS, 16, 256), BF),
            VM((HEADS, 8, PAD), jnp.int32),
            VM((HEADS, 32, PAD), BF),
            VM((HEADS, 8, PAD), jnp.int32),
            VM((HEADS, 32, PAD), F32),
            VM((HEADS, 32, PAD), F32),
            VM((HEADS, 32, 512), BF),
            VM((LEVEL_AT[2] + 128, 128), F32),
            VM((LEVEL_AT[2], 128), F32),
            VM((PAD, 8 * 128), F32),
            VM((PAD, 8 * 128), F32),
            VM((PAD, 128), BF),
            VM((PAD, 128), BF),
            VM((PAD, 128), BF),
            VM((PAD, 128), BF),
            VM((HEADS, 32, PAD), BF),
            VM((HEADS, 32, PAD), BF),
            pltpu.SMEM((8, PAD), jnp.int32),
            pltpu.SMEM((8, PAD), jnp.int32),
            dma((16,)),
            dma((2,)),
            dma((5, NZ)),
            dma((5, NZ)),
            dma((2, 10)),
            dma((2, 10)),
        ],
        compiler_params=pltpu.CompilerParams(
            collective_id=0, has_side_effects=True, vmem_limit_bytes=60 << 20
        ),
        name="layer",
    )(
        features, corners, bilinear, attention, w_value, row(b_value), w_out, row(b_out),
        row(norm1_gain), row(norm1_bias), w_in, row(b_in), w_ffout, row(b_ffout),
        row(norm2_gain), row(norm2_bias),
    )


def solution(mesh):
    split = Mesh(mesh.devices.reshape(mesh.shape["dp"], NY, NZ), DP_BAND)
    return jax.shard_map(
        body,
        mesh=split,
        in_specs=(P(DP_BAND, None),) * 4 + (P(),) * 12,
        out_specs=P(DP_BAND, None),
        check_vma=False,
    )
```

```python
import jax
import jax.numpy as jnp
from jax import lax
from jax.experimental import pallas as pl
from jax.experimental.pallas import tpu as pltpu
from jax.sharding import Mesh
from jax.sharding import PartitionSpec as P

MESH_ID = pl.DeviceIdType.MESH
DP_BAND = ("dp", "band_0", "band_1")
HEADS = 8
NY, NZ = 4, 8
BANDS = NY * NZ
BAND_ROWS = 255
PAD = 256
LEVEL_ROWS = (6144, 1536, 384, 96)
LEVEL_AT = (0, 6144, 7680, 8064)
STRIDE = (128, 64, 32, 16)
BAND_PART = (192, 48, 12, 3)
BAND_AT = (0, 192, 240, 252)
TOKENS = 8160
POINTS = 16
FAR_FIRST = (4, 3, 5, 2, 6, 1, 7)
BF = jnp.bfloat16
F32 = jnp.float32
VM = pltpu.VMEM


def dot(a, b, ca, cb, precision=None):
    return lax.dot_general(
        a, b, (((ca,), (cb,)), ((), ())), preferred_element_type=F32, precision=precision
    )


def onehot(rows, columns, hit):
    r = lax.broadcasted_iota(jnp.int32, (rows, columns), 0)
    c = lax.broadcasted_iota(jnp.int32, (rows, columns), 1)
    return hit(r, c).astype(BF)


def layer_norm(inputs, gain, shift):
    average = jnp.mean(inputs, axis=-1, keepdims=True)
    centred = inputs - average
    variance = jnp.mean(centred * centred, axis=-1, keepdims=True)
    return centred * lax.rsqrt(variance + 1e-05) * gain + shift


def lanes_of(window, lane):
    return lax.gather(
        window,
        lane[..., None],
        lax.GatherDimensionNumbers(
            offset_dims=(),
            collapsed_slice_dims=(1,),
            start_index_map=(1,),
            operand_batching_dims=(0,),
            start_indices_batching_dims=(0,),
        ),
        slice_sizes=(1, 1),
        mode=lax.GatherScatterMode.PROMISE_IN_BOUNDS,
    )


def layer_kernel(
    feat_in, corner_in, bil_in, att_in, w_value_in, b_value_in, w_out_in, b_out_in, gain1_in, shift1_in,
    w_in_in, b_in_in, w_ff_in, b_ff_in, gain2_in, shift2_in,
    out,
    feat, corner, bil, att, w_value, b_value, w_out, b_out, gain1, shift1, w_in, b_in, w_ff, b_ff,
    gain2, shift2, turned_ids,
    send_v, send_s, send_i, send_w, parts, smalls, index, weight, near_i, near_w, near_sum, coarse,
    rows, table, spread_a, spread_b, major_a, major_b, minor_a, minor_b, done, heads, ids_a, ids_b,
    load_sem, ids_sem, sems_out, sems_in, y_out, y_in,
):
    y = lax.axis_index("band_0")
    z = lax.axis_index("band_1")
    here = y * NZ + z
    barrier = pltpu.get_barrier_semaphore()
    for d in range(1, NZ):
        pl.semaphore_signal(
            barrier, inc=1, device_id={"band_1": lax.rem(z + d, NZ)}, device_id_type=MESH_ID
        )
    for d in (1, NY - 1):
        pl.semaphore_signal(
            barrier, inc=1, device_id={"band_0": lax.rem(y + d, NY)}, device_id_type=MESH_ID
        )
    loads = [
        pltpu.make_async_copy(src, dst, load_sem.at[i])
        for i, (src, dst) in enumerate(
            (
                (feat_in, feat), (w_value_in, w_value), (b_value_in, b_value), (corner_in, corner),
                (att_in, att), (bil_in, bil), (w_out_in, w_out), (b_out_in, b_out),
                (gain1_in, gain1), (shift1_in, shift1), (w_in_in, w_in), (b_in_in, b_in),
                (w_ff_in, w_ff), (b_ff_in, b_ff), (gain2_in, gain2), (shift2_in, shift2),
            )
        )
    ]
    for c in loads[0:3]:
        c.start()

    def z_copy(kind, src, dst, slot, d, back=False):
        t = lax.rem(z + NZ - d, NZ) if back else lax.rem(z + d, NZ)
        return pltpu.make_async_remote_copy(
            src_ref=src if src is send_s else src.at[t],
            dst_ref=dst.at[slot],
            send_sem=sems_out.at[kind, d],
            recv_sem=sems_in.at[kind, d],
            device_id={"band_1": t},
            device_id_type=MESH_ID,
        )

    def v_copy(d):
        return z_copy(0, send_v, parts, here, d)

    def i_copy(d):
        return z_copy(1, send_i, index, z, d)

    def w_copy(d):
        return z_copy(2, send_w, weight, z, d)

    def h_copy(d):
        return z_copy(3, done, heads, z, d, back=True)

    def s_copy(d):
        return z_copy(4, send_s, smalls, here, d)

    above, below = lax.rem(y + 1, NY), lax.rem(y + NY - 1, NY)
    legs = (
        (
            (1, y, 0, 4), (1, y, 4, 4), (NY - 1, y, 4, 4), (NY - 1, y, 0, 4),
            (1, below, 0, 4), (NY - 1, above, 4, 4),
        ),
        (
            (1, y, 0, 2), (1, y, 2, 2), (NY - 1, y, 4, 2), (NY - 1, y, 6, 2),
            (1, y, 4, 4), (NY - 1, y, 0, 4),
            (1, below, 0, 2), (NY - 1, above, 4, 2), (1, below, 2, 2), (NY - 1, above, 6, 2),
        ),
    )

    def y_copy(kind, leg):
        step, column, begin, count = legs[kind][leg]
        piece = (smalls, parts)[kind].at[pl.ds(column * NZ + begin, count)]
        return pltpu.make_async_remote_copy(
            src_ref=piece,
            dst_ref=piece,
            send_sem=y_out.at[kind, leg],
            recv_sem=y_in.at[kind, leg],
            device_id={"band_0": lax.rem(y + step, NY)},
            device_id_type=MESH_ID,
        )

    for c in loads[0:3]:
        c.wait()
    for c in loads[3:]:
        c.start()
    values = (dot(feat[...], w_value[...], 1, 0) + b_value[...]).astype(BF)
    eye = onehot(256, 256, lambda r, c: r == c)
    turned = dot(eye, values, 1, 1).astype(BF)
    send_s[...] = jnp.zeros((16, 256), BF)
    send_s[0:15, :] = values[BAND_AT[2] : BAND_ROWS, :]
    send_v[:, :, 0:BAND_ROWS] = turned.reshape(HEADS, 32, BAND_ROWS)
    pl.semaphore_wait(barrier, NZ + 1)
    for d in FAR_FIRST:
        s_copy(d).start()
    for d in FAR_FIRST:
        v_copy(d).start()
    parts[here] = send_v[z]
    smalls[here] = send_s[...]

    loads[3].wait()
    turned_ids[0, :, :] = jnp.transpose(corner[0:128, :])
    turned_ids[1, :, 0 : BAND_ROWS - 128] = jnp.transpose(corner[128:BAND_ROWS, :])
    level = (lax.broadcasted_iota(jnp.int32, (128, 128), 0) // 4) % 4
    base = jnp.where(
        level == 0, LEVEL_AT[0], jnp.where(level == 1, LEVEL_AT[1], jnp.where(level == 2, 0, 384))
    )
    used = lax.broadcasted_iota(jnp.int32, (128, 128), 1) < BAND_ROWS - 128
    left = turned_ids[0, pl.ds(0, 128, stride=4), :] + base
    right = jnp.where(used, turned_ids[1, pl.ds(0, 128, stride=4), :] + base, 0)
    for at, side in ((0, left), (128, right)):
        side = side.reshape(HEADS, POINTS, 128)
        send_i[:, :, at : at + 128] = side[:, 0:8]
        near_i[:, :, at : at + 128] = side[:, 8:16]
    for d in FAR_FIRST:
        i_copy(d).start()
    index[z] = send_i[z]

    loads[4].wait()
    loads[5].wait()
    repeat = onehot(128, 512, lambda r, c: c // 4 == r)
    whole = att[...]
    first = whole.astype(BF)
    rest = whole - first.astype(F32)
    second = rest.astype(BF)
    third = (rest - second.astype(F32)).astype(BF)
    each = dot(first, repeat, 1, 0) + dot(second, repeat, 1, 0) + dot(third, repeat, 1, 0)
    product = (each * bil[...]).astype(BF)
    eye2 = onehot(512, 512, lambda r, c: r == c)
    turned_w = dot(eye2, product, 1, 1).reshape(HEADS, 64, BAND_ROWS)
    send_w[:, :, 0:BAND_ROWS] = turned_w[:, 0:32].astype(BF)
    near_w[:, :, 0:BAND_ROWS] = turned_w[:, 32:64]
    for d in FAR_FIRST:
        w_copy(d).start()
    weight[z] = send_w[z]

    widen = onehot(32, 8 * 128, lambda r, c: c // 32 == r)
    sub = lax.broadcasted_iota(jnp.int32, (8, 128), 0)
    set_a = (spread_a, major_a, minor_a, ids_a, 0)
    set_b = (spread_b, major_b, minor_b, ids_b, 1)

    def owner(d):
        return lax.rem(z + 2 * NZ - 1 - d, NZ)

    def fetch(d, bufs):
        return pltpu.make_async_copy(index.at[owner(d)], bufs[3], ids_sem.at[bufs[4]])

    major_b[...] = jnp.zeros((PAD, 128), BF)
    minor_b[...] = jnp.zeros((PAD, 128), BF)

    for d in range(1, NZ):
        s_copy(d).wait_recv()
    for leg in range(4):
        y_copy(0, leg).start()
    rep = onehot(32, 128, lambda r, c: c % 32 == r)
    for d in range(1, NZ):
        v_copy(d).wait_recv()
    for leg in (0, 2, 1, 3):
        y_copy(1, leg).start()

    def add_rows(column):
        for i in range(NZ):
            b = column * NZ + i
            wide = dot(parts[b], rep, 0, 0)
            for at, count, begin in zip(LEVEL_AT[:2], BAND_PART[:2], BAND_AT[:2]):
                rows[pl.ds(pl.multiple_of(at + b * count, 16), count), :] = wide[
                    begin : begin + count, :
                ]

    def four(start, count, level):
        stride = STRIDE[level]
        lane = lax.broadcasted_iota(jnp.int32, (128, 128), 1)

        def chunk(i, carry):
            k = (start + i) * 128
            k = jnp.where(k >= LEVEL_ROWS[level], k - LEVEL_ROWS[level], k) + LEVEL_AT[level]
            k = pl.multiple_of(k, 128)
            c0 = rows[pl.ds(k, 128), :]
            c1 = rows[pl.ds(k + 1, 128), :]
            c2 = rows[pl.ds(pl.multiple_of(k + stride, 8), 128), :]
            c3 = rows[pl.ds(k + stride + 1, 128), :]
            table[pl.ds(k, 128), :] = jnp.where(
                lane < 64, jnp.where(lane < 32, c0, c1), jnp.where(lane < 96, c2, c3)
            )
            return carry

        lax.fori_loop(0, count, chunk, 0)

    rows[LEVEL_AT[2] : LEVEL_AT[2] + 128, :] = jnp.zeros((128, 128), F32)
    add_rows(y)
    place = lax.broadcasted_iota(jnp.int32, (512, 512), 0)
    spot = lax.broadcasted_iota(jnp.int32, (512, 512), 1)
    inner = place % 16
    goal = jnp.where(
        inner < 12,
        place // 16 * 12 + inner,
        jnp.where(inner < 15, 384 + place // 16 * 3 + inner - 12, -1),
    )
    to_map = (goal == spot).astype(BF)

    for came, leg in ((0, 4), (2, 5)):
        y_copy(0, came).wait_recv()
        y_copy(0, leg).start()
    for leg in (4, 5):
        y_copy(1, leg).start()
    for came, leg in ((0, 6), (2, 7), (1, 8), (3, 9)):
        y_copy(1, came).wait_recv()
        y_copy(1, leg).start()
    i_copy(1).wait_recv()
    fetch(0, set_a).start()
    w_copy(1).wait_recv()
    spread_a[...] = dot(weight[owner(0)], widen, 0, 0)
    for came in (1, 3, 4, 5):
        y_copy(0, came).wait_recv()
    coarse[...] = dot(smalls[...].reshape(512, 256), to_map, 0, 0).astype(BF).reshape(
        HEADS, 32, 512
    )

    def near_head(h, carry):
        for half in range(2):
            at = slice(half * 128, half * 128 + 128)
            sums = [jnp.zeros((16, 128), F32) for _ in range(2)]
            for point in range(8):
                stride = STRIDE[2 + point // 4]
                anchor = jnp.broadcast_to(near_i[h, point : point + 1, at], (16, 128)).astype(
                    jnp.int16
                )
                for c, off in enumerate((0, 1, stride, stride + 1)):
                    spot = anchor + jnp.int16(off)
                    lane = spot & jnp.int16(127)
                    w = jnp.broadcast_to(
                        near_w[h, point * 4 + c : point * 4 + c + 1, at], (16, 128)
                    )
                    for v in range(2):

                        def take(g):
                            return lanes_of(
                                coarse[h, v * 16 : v * 16 + 16, g * 128 : g * 128 + 128], lane
                            )

                        if point >= 4:
                            got = take(3)
                        else:
                            got = jnp.where(
                                spot < 128, take(0), jnp.where(spot < 256, take(1), take(2))
                            )
                        sums[v] = sums[v] + got.astype(F32) * w
            near_sum[h, :, at] = jnp.concatenate(sums, axis=0)
        return carry

    lax.fori_loop(0, 2, near_head, 0)
    for came in (4, 5):
        y_copy(1, came).wait_recv()
    add_rows(lax.rem(y + 1, NY))
    add_rows(lax.rem(y + 3, NY))
    four(lax.rem(y + 3, NY) * 12, 34, 0)
    four(lax.rem(y + 3, NY) * 3, 8, 1)
    for came in (6, 7, 8, 9):
        y_copy(1, came).wait_recv()
    add_rows(lax.rem(y + 2, NY))

    four(lax.rem(y + 1, NY) * 12 + 10, 14, 0)
    four(lax.rem(y + 1, NY) * 3 + 2, 4, 1)

    def close(d, bufs):
        done[owner(d)] = (dot(rep, bufs[1][...], 1, 1) + dot(rep, bufs[2][...], 1, 1)).astype(BF)

    def send_back(d):
        h_copy(d + 1).start()

    def stage(d, bufs, other):
        spread, major, minor, ids, _ = bufs

        @pl.when(d < NZ - 2)
        def _():
            i_copy(d + 2).wait_recv()
            w_copy(d + 2).wait_recv()

        @pl.when(d < NZ - 1)
        def _():
            fetch(d + 1, other).start()

        fetch(d, bufs).wait()

        @pl.when(here + d > -1)
        def _():
            other[0][...] = dot(weight[owner(d + 1)], widen, 0, 0)
            for chunk in range(8):
                total = []
                for q0 in range(chunk * 32, chunk * 32 + 32, 8):
                    acc = None
                    for r in range(8):
                        got = None
                        for k in range(8):
                            one = jnp.broadcast_to(table[pl.ds(ids[r, q0 + k], 1), :], (8, 128))
                            got = one if got is None else jnp.where(sub == k, one, got)
                        term = got * spread[q0 : q0 + 8, r * 128 : r * 128 + 128]
                        acc = term if acc is None else acc + term
                    total.append(acc)
                total = jnp.concatenate(total, axis=0)
                top = total.astype(BF)
                major[chunk * 32 : chunk * 32 + 32, :] = top
                minor[chunk * 32 : chunk * 32 + 32, :] = (total - top.astype(F32)).astype(BF)
            close(d - 1, other)

    def pair(i, carry):
        d = 2 * i
        stage(d, set_a, set_b)

        @pl.when(i > 0)
        def _():
            send_back(d - 1)

        stage(d + 1, set_b, set_a)
        send_back(d)
        return carry

    lax.fori_loop(0, NZ // 2, pair, 0)
    close(NZ - 1, set_b)
    heads[z] = done[z]

    lax.fori_loop(2, HEADS, near_head, 0)
    for c in loads[6:]:
        c.wait()
    for d in range(1, NZ):
        h_copy(d).wait_recv()
    sampled = (
        heads[...].reshape(256, PAD).astype(F32) + near_sum[...].reshape(256, PAD)
    ).astype(BF)
    attended = dot(sampled, w_out[...], 0, 0)[0:BAND_ROWS] + b_out[...]
    middle = layer_norm(feat[...].astype(F32) + attended, gain1[...], shift1[...]).astype(BF)
    hidden = jnp.maximum(dot(middle, w_in[...], 1, 0) + b_in[...], 0.0).astype(BF)
    result = middle.astype(F32) + dot(hidden, w_ff[...], 1, 0) + b_ff[...]
    out[...] = layer_norm(result, gain2[...], shift2[...]).astype(BF)
    for d in range(1, NZ):
        for c in (v_copy(d), i_copy(d), w_copy(d), h_copy(d), s_copy(d)):
            c.wait_send()
    for kind in range(2):
        for leg in range(len(legs[kind])):
            y_copy(kind, leg).wait_send()


def body(
    features, corners, bilinear, attention, w_value, b_value, w_out, b_out,
    norm1_gain, norm1_bias, w_in, b_in, w_ffout, b_ffout, norm2_gain, norm2_bias,
):
    def row(x):
        return x.reshape(1, -1)

    def like(x):
        return VM(x.shape, x.dtype)

    def flat(n):
        return VM((1, n), F32)

    dma = pltpu.SemaphoreType.DMA
    vec = pl.BlockSpec(memory_space=VM)
    return pl.pallas_call(
        layer_kernel,
        out_shape=jax.ShapeDtypeStruct((BAND_ROWS, 256), BF),
        in_specs=[pl.BlockSpec(memory_space=pl.ANY)] * 16,
        out_specs=vec,
        scratch_shapes=[
            like(features), like(corners), like(bilinear), like(attention), like(w_value), flat(256),
            like(w_out), flat(256), flat(256), flat(256), like(w_in), flat(1024), like(w_ffout),
            flat(256), flat(256), flat(256),
            VM((2, 512, 128), jnp.int32),
            VM((HEADS, 32, PAD), BF),
            VM((16, 256), BF),
            VM((HEADS, 8, PAD), jnp.int32),
            VM((HEADS, 32, PAD), BF),
            VM((BANDS, 32, PAD), BF),
            VM((BANDS, 16, 256), BF),
            VM((HEADS, 8, PAD), jnp.int32),
            VM((HEADS, 32, PAD), BF),
            VM((HEADS, 8, PAD), jnp.int32),
            VM((HEADS, 32, PAD), F32),
            VM((HEADS, 32, PAD), F32),
            VM((HEADS, 32, 512), BF),
            VM((LEVEL_AT[2] + 128, 128), F32),
            VM((LEVEL_AT[2], 128), F32),
            VM((PAD, 8 * 128), F32),
            VM((PAD, 8 * 128), F32),
            VM((PAD, 128), BF),
            VM((PAD, 128), BF),
            VM((PAD, 128), BF),
            VM((PAD, 128), BF),
            VM((HEADS, 32, PAD), BF),
            VM((HEADS, 32, PAD), BF),
            pltpu.SMEM((8, PAD), jnp.int32),
            pltpu.SMEM((8, PAD), jnp.int32),
            dma((16,)),
            dma((2,)),
            dma((5, NZ)),
            dma((5, NZ)),
            dma((2, 10)),
            dma((2, 10)),
        ],
        compiler_params=pltpu.CompilerParams(
            collective_id=0, has_side_effects=True, vmem_limit_bytes=60 << 20
        ),
        name="layer",
    )(
        features, corners, bilinear, attention, w_value, row(b_value), w_out, row(b_out),
        row(norm1_gain), row(norm1_bias), w_in, row(b_in), w_ffout, row(b_ffout),
        row(norm2_gain), row(norm2_bias),
    )


def solution(mesh):
    split = Mesh(mesh.devices.reshape(mesh.shape["dp"], NY, NZ), DP_BAND)
    return jax.shard_map(
        body,
        mesh=split,
        in_specs=(P(DP_BAND, None),) * 4 + (P(),) * 12,
        out_specs=P(DP_BAND, None),
        check_vma=False,
    )
```

```python
import jax
import jax.numpy as jnp
from jax import lax
from jax.experimental import pallas as pl
from jax.experimental.pallas import tpu as pltpu
from jax.sharding import Mesh
from jax.sharding import PartitionSpec as P

MESH_ID = pl.DeviceIdType.MESH
DP_BAND = ("dp", "band_0", "band_1")
HEADS = 8
NY, NZ = 4, 8
BANDS = NY * NZ
BAND_ROWS = 255
PAD = 256
LEVEL_ROWS = (6144, 1536, 384, 96)
LEVEL_AT = (0, 6144, 7680, 8064)
STRIDE = (128, 64, 32, 16)
BAND_PART = (192, 48, 12, 3)
BAND_AT = (0, 192, 240, 252)
TOKENS = 8160
POINTS = 16
FAR_FIRST = (4, 3, 5, 2, 6, 1, 7)
BF = jnp.bfloat16
F32 = jnp.float32
VM = pltpu.VMEM


def dot(a, b, ca, cb, precision=None):
    return lax.dot_general(
        a, b, (((ca,), (cb,)), ((), ())), preferred_element_type=F32, precision=precision
    )


def onehot(rows, columns, hit):
    r = lax.broadcasted_iota(jnp.int32, (rows, columns), 0)
    c = lax.broadcasted_iota(jnp.int32, (rows, columns), 1)
    return hit(r, c).astype(BF)


def layer_norm(inputs, gain, shift):
    average = jnp.mean(inputs, axis=-1, keepdims=True)
    centred = inputs - average
    variance = jnp.mean(centred * centred, axis=-1, keepdims=True)
    return centred * lax.rsqrt(variance + 1e-05) * gain + shift


def lanes_of(window, lane):
    return lax.gather(
        window,
        lane[..., None],
        lax.GatherDimensionNumbers(
            offset_dims=(),
            collapsed_slice_dims=(1,),
            start_index_map=(1,),
            operand_batching_dims=(0,),
            start_indices_batching_dims=(0,),
        ),
        slice_sizes=(1, 1),
        mode=lax.GatherScatterMode.PROMISE_IN_BOUNDS,
    )


def layer_kernel(
    feat_in, corner_in, bil_in, att_in, w_value_in, b_value_in, w_out_in, b_out_in, gain1_in, shift1_in,
    w_in_in, b_in_in, w_ff_in, b_ff_in, gain2_in, shift2_in,
    out,
    feat, corner, bil, att, w_value, b_value, w_out, b_out, gain1, shift1, w_in, b_in, w_ff, b_ff,
    gain2, shift2, turned_ids,
    send_v, send_s, send_i, send_w, parts, smalls, index, weight, near_i, near_w, near_sum, coarse,
    rows, table, spread_a, spread_b, major_a, major_b, minor_a, minor_b, done, heads, ids_a, ids_b,
    load_sem, ids_sem, sems_out, sems_in, y_out, y_in,
):
    y = lax.axis_index("band_0")
    z = lax.axis_index("band_1")
    here = y * NZ + z
    barrier = pltpu.get_barrier_semaphore()
    for d in range(1, NZ):
        pl.semaphore_signal(
            barrier, inc=1, device_id={"band_1": lax.rem(z + d, NZ)}, device_id_type=MESH_ID
        )
    for d in (1, NY - 1):
        pl.semaphore_signal(
            barrier, inc=1, device_id={"band_0": lax.rem(y + d, NY)}, device_id_type=MESH_ID
        )
    loads = [
        pltpu.make_async_copy(src, dst, load_sem.at[i])
        for i, (src, dst) in enumerate(
            (
                (feat_in, feat), (w_value_in, w_value), (b_value_in, b_value), (corner_in, corner),
                (att_in, att), (bil_in, bil), (w_out_in, w_out), (b_out_in, b_out),
                (gain1_in, gain1), (shift1_in, shift1), (w_in_in, w_in), (b_in_in, b_in),
                (w_ff_in, w_ff), (b_ff_in, b_ff), (gain2_in, gain2), (shift2_in, shift2),
            )
        )
    ]
    for c in loads[0:3]:
        c.start()

    def z_copy(kind, src, dst, slot, d, back=False):
        t = lax.rem(z + NZ - d, NZ) if back else lax.rem(z + d, NZ)
        return pltpu.make_async_remote_copy(
            src_ref=src if src is send_s else src.at[t],
            dst_ref=dst.at[slot],
            send_sem=sems_out.at[kind, d],
            recv_sem=sems_in.at[kind, d],
            device_id={"band_1": t},
            device_id_type=MESH_ID,
        )

    def v_copy(d):
        return z_copy(0, send_v, parts, here, d)

    def i_copy(d):
        return z_copy(1, send_i, index, z, d)

    def w_copy(d):
        return z_copy(2, send_w, weight, z, d)

    def h_copy(d):
        return z_copy(3, done, heads, z, d, back=True)

    def s_copy(d):
        return z_copy(4, send_s, smalls, here, d)

    above, below = lax.rem(y + 1, NY), lax.rem(y + NY - 1, NY)
    legs = (
        (
            (1, y, 0, 4), (1, y, 4, 4), (NY - 1, y, 4, 4), (NY - 1, y, 0, 4),
            (1, below, 0, 4), (NY - 1, above, 4, 4),
        ),
        (
            (1, y, 0, 2), (1, y, 2, 2), (NY - 1, y, 4, 2), (NY - 1, y, 6, 2),
            (1, y, 4, 4), (NY - 1, y, 0, 4),
            (1, below, 0, 2), (NY - 1, above, 4, 2), (1, below, 2, 2), (NY - 1, above, 6, 2),
        ),
    )

    def y_copy(kind, leg):
        step, column, begin, count = legs[kind][leg]
        piece = (smalls, parts)[kind].at[pl.ds(column * NZ + begin, count)]
        return pltpu.make_async_remote_copy(
            src_ref=piece,
            dst_ref=piece,
            send_sem=y_out.at[kind, leg],
            recv_sem=y_in.at[kind, leg],
            device_id={"band_0": lax.rem(y + step, NY)},
            device_id_type=MESH_ID,
        )

    for c in loads[0:3]:
        c.wait()
    for c in loads[3:]:
        c.start()
    values = (dot(feat[...], w_value[...], 1, 0) + b_value[...]).astype(BF)
    eye = onehot(256, 256, lambda r, c: r == c)
    turned = dot(eye, values, 1, 1).astype(BF)
    send_s[...] = jnp.zeros((16, 256), BF)
    send_s[0:15, :] = values[BAND_AT[2] : BAND_ROWS, :]
    send_v[:, :, 0:BAND_ROWS] = turned.reshape(HEADS, 32, BAND_ROWS)
    pl.semaphore_wait(barrier, NZ + 1)
    for d in FAR_FIRST:
        s_copy(d).start()
    for d in FAR_FIRST:
        v_copy(d).start()
    parts[here] = send_v[z]
    smalls[here] = send_s[...]

    loads[3].wait()
    turned_ids[0, :, :] = jnp.transpose(corner[0:128, :])
    turned_ids[1, :, 0 : BAND_ROWS - 128] = jnp.transpose(corner[128:BAND_ROWS, :])
    level = (lax.broadcasted_iota(jnp.int32, (128, 128), 0) // 4) % 4
    base = jnp.where(
        level == 0, LEVEL_AT[0], jnp.where(level == 1, LEVEL_AT[1], jnp.where(level == 2, 0, 384))
    )
    used = lax.broadcasted_iota(jnp.int32, (128, 128), 1) < BAND_ROWS - 128
    left = turned_ids[0, pl.ds(0, 128, stride=4), :] + base
    right = jnp.where(used, turned_ids[1, pl.ds(0, 128, stride=4), :] + base, 0)
    for at, side in ((0, left), (128, right)):
        side = side.reshape(HEADS, POINTS, 128)
        send_i[:, :, at : at + 128] = side[:, 0:8]
        near_i[:, :, at : at + 128] = side[:, 8:16]
    for d in FAR_FIRST:
        i_copy(d).start()
    index[z] = send_i[z]

    loads[4].wait()
    loads[5].wait()
    repeat = onehot(128, 512, lambda r, c: c // 4 == r)
    whole = att[...]
    first = whole.astype(BF)
    rest = whole - first.astype(F32)
    second = rest.astype(BF)
    third = (rest - second.astype(F32)).astype(BF)
    each = dot(first, repeat, 1, 0) + dot(second, repeat, 1, 0) + dot(third, repeat, 1, 0)
    product = (each * bil[...]).astype(BF)
    eye2 = onehot(512, 512, lambda r, c: r == c)
    turned_w = dot(eye2, product, 1, 1).reshape(HEADS, 64, BAND_ROWS)
    send_w[:, :, 0:BAND_ROWS] = turned_w[:, 0:32].astype(BF)
    near_w[:, :, 0:BAND_ROWS] = turned_w[:, 32:64]
    for d in FAR_FIRST:
        w_copy(d).start()
    weight[z] = send_w[z]

    widen = onehot(32, 8 * 128, lambda r, c: c // 32 == r)
    sub = lax.broadcasted_iota(jnp.int32, (8, 128), 0)
    set_a = (spread_a, major_a, minor_a, ids_a, 0)
    set_b = (spread_b, major_b, minor_b, ids_b, 1)

    def owner(d):
        return lax.rem(z + 2 * NZ - 1 - d, NZ)

    def fetch(d, bufs):
        return pltpu.make_async_copy(index.at[owner(d)], bufs[3], ids_sem.at[bufs[4]])

    major_b[...] = jnp.zeros((PAD, 128), BF)
    minor_b[...] = jnp.zeros((PAD, 128), BF)

    for d in range(1, NZ):
        s_copy(d).wait_recv()
    for leg in range(4):
        y_copy(0, leg).start()
    rep = onehot(32, 128, lambda r, c: c % 32 == r)
    for d in range(1, NZ):
        v_copy(d).wait_recv()
    for leg in (0, 2, 1, 3):
        y_copy(1, leg).start()

    def add_rows(column):
        for i in range(NZ):
            b = column * NZ + i
            wide = dot(parts[b], rep, 0, 0)
            for at, count, begin in zip(LEVEL_AT[:2], BAND_PART[:2], BAND_AT[:2]):
                rows[pl.ds(pl.multiple_of(at + b * count, 16), count), :] = wide[
                    begin : begin + count, :
                ]

    def four(start, count, level):
        stride = STRIDE[level]
        lane = lax.broadcasted_iota(jnp.int32, (128, 128), 1)

        def chunk(i, carry):
            k = (start + i) * 128
            k = jnp.where(k >= LEVEL_ROWS[level], k - LEVEL_ROWS[level], k) + LEVEL_AT[level]
            k = pl.multiple_of(k, 128)
            c0 = rows[pl.ds(k, 128), :]
            c1 = rows[pl.ds(k + 1, 128), :]
            c2 = rows[pl.ds(pl.multiple_of(k + stride, 8), 128), :]
            c3 = rows[pl.ds(k + stride + 1, 128), :]
            table[pl.ds(k, 128), :] = jnp.where(
                lane < 64, jnp.where(lane < 32, c0, c1), jnp.where(lane < 96, c2, c3)
            )
            return carry

        lax.fori_loop(0, count, chunk, 0)

    rows[LEVEL_AT[2] : LEVEL_AT[2] + 128, :] = jnp.zeros((128, 128), F32)
    add_rows(y)
    place = lax.broadcasted_iota(jnp.int32, (512, 512), 0)
    spot = lax.broadcasted_iota(jnp.int32, (512, 512), 1)
    inner = place % 16
    goal = jnp.where(
        inner < 12,
        place // 16 * 12 + inner,
        jnp.where(inner < 15, 384 + place // 16 * 3 + inner - 12, -1),
    )
    to_map = (goal == spot).astype(BF)

    for came, leg in ((0, 4), (2, 5)):
        y_copy(0, came).wait_recv()
        y_copy(0, leg).start()
    for leg in (4, 5):
        y_copy(1, leg).start()
    for came, leg in ((0, 6), (2, 7), (1, 8), (3, 9)):
        y_copy(1, came).wait_recv()
        y_copy(1, leg).start()
    i_copy(1).wait_recv()
    fetch(0, set_a).start()
    w_copy(1).wait_recv()
    spread_a[...] = dot(weight[owner(0)], widen, 0, 0)
    for came in (1, 3, 4, 5):
        y_copy(0, came).wait_recv()
    coarse[...] = dot(smalls[...].reshape(512, 256), to_map, 0, 0).astype(BF).reshape(
        HEADS, 32, 512
    )

    def near_head(h, carry):
        for half in range(2):
            at = slice(half * 128, half * 128 + 128)
            sums = [jnp.zeros((16, 128), F32) for _ in range(2)]
            for point in range(8):
                stride = STRIDE[2 + point // 4]
                anchor = jnp.broadcast_to(near_i[h, point : point + 1, at], (16, 128)).astype(
                    jnp.int16
                )
                for c, off in enumerate((0, 1, stride, stride + 1)):
                    spot = anchor + jnp.int16(off)
                    lane = spot & jnp.int16(127)
                    w = jnp.broadcast_to(
                        near_w[h, point * 4 + c : point * 4 + c + 1, at], (16, 128)
                    )
                    for v in range(2):

                        def take(g):
                            return lanes_of(
                                coarse[h, v * 16 : v * 16 + 16, g * 128 : g * 128 + 128], lane
                            )

                        if point >= 4:
                            got = take(3)
                        else:
                            got = jnp.where(
                                spot < 128, take(0), jnp.where(spot < 256, take(1), take(2))
                            )
                        sums[v] = sums[v] + got.astype(F32) * w
            near_sum[h, :, at] = jnp.concatenate(sums, axis=0)
        return carry

    lax.fori_loop(0, 1, near_head, 0)
    for came in (4, 5):
        y_copy(1, came).wait_recv()
    add_rows(lax.rem(y + 1, NY))
    add_rows(lax.rem(y + 3, NY))
    four(lax.rem(y + 3, NY) * 12, 34, 0)
    four(lax.rem(y + 3, NY) * 3, 8, 1)
    for came in (6, 7, 8, 9):
        y_copy(1, came).wait_recv()
    add_rows(lax.rem(y + 2, NY))

    four(lax.rem(y + 1, NY) * 12 + 10, 14, 0)
    four(lax.rem(y + 1, NY) * 3 + 2, 4, 1)

    def close(d, bufs):
        done[owner(d)] = (dot(rep, bufs[1][...], 1, 1) + dot(rep, bufs[2][...], 1, 1)).astype(BF)

    def send_back(d):
        h_copy(d + 1).start()

    def stage(d, bufs, other):
        spread, major, minor, ids, _ = bufs

        @pl.when(d < NZ - 2)
        def _():
            i_copy(d + 2).wait_recv()
            w_copy(d + 2).wait_recv()

        @pl.when(d < NZ - 1)
        def _():
            fetch(d + 1, other).start()

        fetch(d, bufs).wait()

        @pl.when(here + d > -1)
        def _():
            other[0][...] = dot(weight[owner(d + 1)], widen, 0, 0)
            for chunk in range(8):
                total = []
                for q0 in range(chunk * 32, chunk * 32 + 32, 8):
                    acc = None
                    for r in range(8):
                        got = None
                        for k in range(8):
                            one = jnp.broadcast_to(table[pl.ds(ids[r, q0 + k], 1), :], (8, 128))
                            got = one if got is None else jnp.where(sub == k, one, got)
                        term = got * spread[q0 : q0 + 8, r * 128 : r * 128 + 128]
                        acc = term if acc is None else acc + term
                    total.append(acc)
                total = jnp.concatenate(total, axis=0)
                top = total.astype(BF)
                major[chunk * 32 : chunk * 32 + 32, :] = top
                minor[chunk * 32 : chunk * 32 + 32, :] = (total - top.astype(F32)).astype(BF)
            close(d - 1, other)

    def pair(i, carry):
        d = 2 * i
        stage(d, set_a, set_b)

        @pl.when(i > 0)
        def _():
            send_back(d - 1)

        stage(d + 1, set_b, set_a)
        send_back(d)
        return carry

    lax.fori_loop(0, NZ // 2, pair, 0)
    close(NZ - 1, set_b)
    heads[z] = done[z]

    lax.fori_loop(1, HEADS, near_head, 0)
    for c in loads[6:]:
        c.wait()
    for d in range(1, NZ):
        h_copy(d).wait_recv()
    sampled = (
        heads[...].reshape(256, PAD).astype(F32) + near_sum[...].reshape(256, PAD)
    ).astype(BF)
    attended = dot(sampled, w_out[...], 0, 0)[0:BAND_ROWS] + b_out[...]
    middle = layer_norm(feat[...].astype(F32) + attended, gain1[...], shift1[...]).astype(BF)
    hidden = jnp.maximum(dot(middle, w_in[...], 1, 0) + b_in[...], 0.0).astype(BF)
    result = middle.astype(F32) + dot(hidden, w_ff[...], 1, 0) + b_ff[...]
    out[...] = layer_norm(result, gain2[...], shift2[...]).astype(BF)
    for d in range(1, NZ):
        for c in (v_copy(d), i_copy(d), w_copy(d), h_copy(d), s_copy(d)):
            c.wait_send()
    for kind in range(2):
        for leg in range(len(legs[kind])):
            y_copy(kind, leg).wait_send()


def body(
    features, corners, bilinear, attention, w_value, b_value, w_out, b_out,
    norm1_gain, norm1_bias, w_in, b_in, w_ffout, b_ffout, norm2_gain, norm2_bias,
):
    def row(x):
        return x.reshape(1, -1)

    def like(x):
        return VM(x.shape, x.dtype)

    def flat(n):
        return VM((1, n), F32)

    dma = pltpu.SemaphoreType.DMA
    vec = pl.BlockSpec(memory_space=VM)
    return pl.pallas_call(
        layer_kernel,
        out_shape=jax.ShapeDtypeStruct((BAND_ROWS, 256), BF),
        in_specs=[pl.BlockSpec(memory_space=pl.ANY)] * 16,
        out_specs=vec,
        scratch_shapes=[
            like(features), like(corners), like(bilinear), like(attention), like(w_value), flat(256),
            like(w_out), flat(256), flat(256), flat(256), like(w_in), flat(1024), like(w_ffout),
            flat(256), flat(256), flat(256),
            VM((2, 512, 128), jnp.int32),
            VM((HEADS, 32, PAD), BF),
            VM((16, 256), BF),
            VM((HEADS, 8, PAD), jnp.int32),
            VM((HEADS, 32, PAD), BF),
            VM((BANDS, 32, PAD), BF),
            VM((BANDS, 16, 256), BF),
            VM((HEADS, 8, PAD), jnp.int32),
            VM((HEADS, 32, PAD), BF),
            VM((HEADS, 8, PAD), jnp.int32),
            VM((HEADS, 32, PAD), F32),
            VM((HEADS, 32, PAD), F32),
            VM((HEADS, 32, 512), BF),
            VM((LEVEL_AT[2] + 128, 128), F32),
            VM((LEVEL_AT[2], 128), F32),
            VM((PAD, 8 * 128), F32),
            VM((PAD, 8 * 128), F32),
            VM((PAD, 128), BF),
            VM((PAD, 128), BF),
            VM((PAD, 128), BF),
            VM((PAD, 128), BF),
            VM((HEADS, 32, PAD), BF),
            VM((HEADS, 32, PAD), BF),
            pltpu.SMEM((8, PAD), jnp.int32),
            pltpu.SMEM((8, PAD), jnp.int32),
            dma((16,)),
            dma((2,)),
            dma((5, NZ)),
            dma((5, NZ)),
            dma((2, 10)),
            dma((2, 10)),
        ],
        compiler_params=pltpu.CompilerParams(
            collective_id=0, has_side_effects=True, vmem_limit_bytes=60 << 20
        ),
        name="layer",
    )(
        features, corners, bilinear, attention, w_value, row(b_value), w_out, row(b_out),
        row(norm1_gain), row(norm1_bias), w_in, row(b_in), w_ffout, row(b_ffout),
        row(norm2_gain), row(norm2_bias),
    )


def solution(mesh):
    split = Mesh(mesh.devices.reshape(mesh.shape["dp"], NY, NZ), DP_BAND)
    return jax.shard_map(
        body,
        mesh=split,
        in_specs=(P(DP_BAND, None),) * 4 + (P(),) * 12,
        out_specs=P(DP_BAND, None),
        check_vma=False,
    )
```
